128 devices in a mesh: seq: 16 (over z, y_hi, core), span: 8 (over x, y_lo).
Axes of the slice: x: 4, y: 4 (y_hi: 2, y_lo: 2; y = y_hi * 2 + y_lo), z: 4, core: 2. Of those that a mesh axis runs over, the one named last changes fastest.
Arguments:
- q_prefill: bfloat16 [8, 2048, 64, 192], P('span', 'seq'), may hold values from -3000 to 3000
- kv_latent: bfloat16 [8, 2048, 512], P('span', 'seq'), may hold values from -200 to 200
- key_rope: bfloat16 [8, 2048, 64], P('span', 'seq'), may hold values from -6 to 6
- segment_ids: int32 [8, 2048], replicated, may hold values from 0 to 15, never falling along the last dimension, each value on 1 to 1024 neighbouring positions
- assignment: int32 [128], replicated, may hold values from 0 to 127, each once
- absorb_key: bfloat16 [64, 128, 512], replicated, may hold values from -0.5 to 0.5
- absorb_value: bfloat16 [64, 512, 128], replicated, may hold values from -0.25 to 0.25
- q_decode: bfloat16 [2, 128, 64, 192], P(None, 'span'), may hold values from -3000 to 3000
- new_latent: bfloat16 [2, 128, 512], P(None, 'span'), may hold values from -6 to 6
- new_rope: bfloat16 [2, 128, 64], P(None, 'span'), may hold values from -6 to 6
Outputs:
- prefill_out: bfloat16 [8, 2048, 8192], P('span', 'seq')
- decode_out: bfloat16 [2, 128, 8192], P(None, 'span')
The draws below stay inside these ranges and needn't reach their ends.
Inputs may be any that keep to these rules, and one draw needn't show every extreme that they name: `segment_ids`: within a span the numbers never fall; each of the 16 numbers appears, on 1 to 1024 positions. `assignment`: each sequence number appears once; entry c * 16 + d is the sequence of prompt d of span c, and sequence g is decoded at span index g // 16, slot g % 16.
All inputs are finite; a program needn't handle non-finite values.
Results may differ from the reference program's by a relative error of at most 0.014.
Values may be sent and summed in bfloat16 or wider, within the bound.
A program may use at most 192 MiB of HBM per device.

```python
import math
import jax
import jax.numpy as jnp
import numpy as np
from jax import lax

H = 64
NOPE = 128
ROPE = 64
LAT = 512
VHEAD = 128
DOCS = 16
STEPS = 2
LEN = 2048
SPANS = 8
SEQS = 128
MOST = 1024


def prefill_align(key):
    base = jax.random.fold_in(key, 7001)
    first = jax.random.fold_in(base, 0)
    rope = jnp.clip(jax.random.normal(first, (SPANS, LEN, ROPE), jnp.float32), -6.0, 6.0)
    return rope


def decode_align(key):
    base = jax.random.fold_in(key, 7003)
    first = jax.random.fold_in(base, 0)
    rope = jnp.clip(jax.random.normal(first, (STEPS, SEQS, ROPE), jnp.float32), -6.0, 6.0)
    return rope


def draw_key_rope(key, part):
    rope = prefill_align(key)
    return rope.astype(jnp.bfloat16)


def draw_q_prefill(key, part):
    base = jax.random.fold_in(key, 7002)
    query = jnp.clip(jax.random.normal(base, (SPANS, LEN, H, NOPE + ROPE), jnp.float32), -6.0, 6.0)
    return query.astype(jnp.bfloat16)


def draw_new_rope(key, part):
    rope = decode_align(key)
    return rope.astype(jnp.bfloat16)


def draw_q_decode(key, part):
    base = jax.random.fold_in(key, 7004)
    query = jnp.clip(jax.random.normal(base, (STEPS, SEQS, H, NOPE + ROPE), jnp.float32), -6.0, 6.0)
    return query.astype(jnp.bfloat16)


def draw_kv_latent(key, part):
    base = jax.random.fold_in(key, 7005)
    first = jax.random.fold_in(base, 0)
    values = jnp.clip(jax.random.normal(first, (SPANS, LEN, LAT), jnp.float32), -6.0, 6.0)
    return values.astype(jnp.bfloat16)


def block_scale(own_key, dims, cuts, least, top_value):
    factor_of, own = 1.0, jax.random.fold_in(own_key, 6)
    for axis_at, parts in cuts:
        steps = jnp.exp(jax.random.uniform(jax.random.fold_in(own, axis_at), (parts,), jnp.float32, least / len(cuts), top_value / len(cuts)))
        factor_of = factor_of * jnp.repeat(steps, dims[axis_at] // parts).reshape([-1 if axis == axis_at else 1 for axis in range(len(dims))])
    return factor_of


def length_profile(number_of, total, limit, slope):
    weights = [(1 << 20) // math.isqrt(rank ** slope) + 1 for rank in range(2, number_of + 1)]
    spare, given = total - limit - (number_of - 1), [1] * (number_of - 1)
    while spare > 0:
        candidates = [i for i in range(number_of - 1) if given[i] < limit]
        mass, remaining = sum([weights[i] for i in candidates]), spare
        for i in candidates:
            more = min(limit - given[i], max(1, remaining * weights[i] // mass), spare)
            given[i] = given[i] + more
            spare = spare - more
    return np.array([limit] + given)


def ragged(stream_key, count, total, reach, skew):
    if count == 2:
        one = jax.random.randint(stream_key, (), max(1, total - reach), min(reach, total - 1) + 1)
        return jnp.stack([one, total - one])
    tallies = jnp.asarray(length_profile(count, total, reach, skew), jnp.int32)
    couples = (count - 1) // 2
    giver, taker = tallies[1:1 + 2 * couples:2], tallies[2:2 + 2 * couples:2]
    slack = jnp.minimum(giver - 1, reach - taker)
    shifted = jax.random.randint(jax.random.fold_in(stream_key, 1), (couples,), 0, 1 << 20) % (slack + 1)
    tallies = tallies.at[1:1 + 2 * couples:2].set(giver - shifted).at[2:2 + 2 * couples:2].set(taker + shifted)
    return tallies[jax.random.permutation(jax.random.fold_in(stream_key, 2), count)]


def bell_draw(rng, shape, deviation, limit, cuts=(), kind=jnp.bfloat16):
    values = jax.random.normal(rng, shape, jnp.float32) * deviation
    if len(cuts) > 0:
        values = block_scale(rng, shape, cuts, -0.22, 0.18) * values
    return jnp.clip(values, min=-limit, max=limit).astype(kind)


def setup_inputs(seed: int = 0) -> dict:
    arg_keys = jax.random.split(jax.random.key(seed), 11)
    return {
        "q_prefill": draw_q_prefill(jax.random.fold_in(arg_keys[10], 71), 0),
        "kv_latent": draw_kv_latent(jax.random.fold_in(arg_keys[10], 71), 0),
        "key_rope": draw_key_rope(jax.random.fold_in(arg_keys[10], 71), 0),
        "segment_ids": jax.vmap(lambda own: jnp.searchsorted(jnp.cumsum(ragged(own, DOCS, LEN, MOST, 2)), jnp.arange(LEN), side="right"))(jax.random.split(arg_keys[3], SPANS)).reshape((SPANS, LEN)).astype(jnp.int32),
        "assignment": jax.random.permutation(arg_keys[4], SEQS).astype(jnp.int32),
        "absorb_key": bell_draw(arg_keys[5], (H, NOPE, LAT), NOPE ** -0.5, 0.5),
        "absorb_value": bell_draw(arg_keys[6], (H, LAT, VHEAD), LAT ** -0.5, 0.25),
        "q_decode": draw_q_decode(jax.random.fold_in(arg_keys[10], 71), 0),
        "new_latent": bell_draw(arg_keys[8], (STEPS, SEQS, LAT), 1.0, 6.0, ((1, 8),)),
        "new_rope": draw_new_rope(jax.random.fold_in(arg_keys[10], 71), 0),
    }


def make_cache(latent, rope):
    values = latent.astype(jnp.float32)
    normed = values * lax.rsqrt(lax.optimization_barrier(jnp.mean(values * values, axis=-1, keepdims=True)) + 1e-06)
    return jnp.concatenate([normed, rope.astype(jnp.float32)], axis=-1).astype(jnp.bfloat16)

def absorb(query, absorb_key):
    latent = jnp.einsum('...hd,hdc->...hc', query[..., :NOPE].astype(jnp.float32), absorb_key.astype(jnp.float32))
    return jnp.concatenate([latent.astype(jnp.bfloat16), query[..., NOPE:]], axis=-1)

def project(latent_out, absorb_value):
    result = jnp.einsum('...hc,hcv->...hv', latent_out.astype(jnp.float32), absorb_value.astype(jnp.float32))
    return result.astype(jnp.bfloat16)

def reference(q_prefill, kv_latent, key_rope, segment_ids, assignment, absorb_key, absorb_value, q_decode, new_latent, new_rope):
    scale = (NOPE + ROPE) ** (-0.5)
    block = LEN // 4

    def prefill_span(args):
        query, latent, rope, seg = args
        cache = make_cache(latent, rope)
        queries = absorb(query, absorb_key)
        pieces = []
        for index in range(4):
            start = index * block
            end = start + block
            keys = cache[:end].astype(jnp.float32)
            scores = jnp.einsum('thc,kc->thk', queries[start:end].astype(jnp.float32), keys) * scale
            pos_q = start + jnp.arange(block, dtype=jnp.int32)
            pos_k = jnp.arange(end, dtype=jnp.int32)
            mask = (seg[start:end, None] == seg[None, :end]) & (pos_q[:, None] >= pos_k[None, :])
            scores = jnp.where(mask[:, None, :], scores, -jnp.inf)
            best = lax.optimization_barrier(jnp.max(scores, axis=-1, keepdims=True))
            weights = jnp.exp(scores - best)
            total = lax.optimization_barrier(jnp.sum(weights, axis=-1))
            accum = jnp.einsum('thk,kc->thc', weights.astype(jnp.bfloat16).astype(jnp.float32), keys[:, :LAT])
            latent_out = (accum / total[..., None]).astype(jnp.bfloat16)
            pieces.append(project(latent_out, absorb_value).reshape(block, H * VHEAD))
        return jnp.concatenate(pieces, axis=0)
    prefill_out = lax.map(prefill_span, (q_prefill, kv_latent, key_rope, segment_ids))

    def decode_span(args):
        queries, fresh_latent, fresh_rope, latent, rope, seg = args
        cache = make_cache(latent, rope).astype(jnp.float32)
        fresh = make_cache(fresh_latent, fresh_rope).astype(jnp.float32)
        dq = absorb(queries, absorb_key).astype(jnp.float32)
        old = jnp.einsum('sdhc,kc->sdhk', dq, cache) * scale
        old_mask = (seg[None, :] == jnp.arange(DOCS, dtype=jnp.int32)[:, None])[None, :, None, :]
        new = jnp.einsum('sdhc,udc->sdhu', dq, fresh) * scale
        steps = jnp.arange(STEPS, dtype=jnp.int32)
        new_mask = (steps[None, :] <= steps[:, None])[:, None, None, :]
        old = jnp.where(old_mask, old, -jnp.inf)
        new = jnp.where(new_mask, new, -jnp.inf)
        best = jnp.maximum(lax.optimization_barrier(jnp.max(old, axis=-1)), lax.optimization_barrier(jnp.max(new, axis=-1)))[..., None]
        old_w = jnp.exp(old - best)
        new_w = jnp.exp(new - best)
        total = lax.optimization_barrier(jnp.sum(old_w, axis=-1)) + lax.optimization_barrier(jnp.sum(new_w, axis=-1))
        accum = jnp.einsum('sdhk,kc->sdhc', old_w.astype(jnp.bfloat16).astype(jnp.float32), cache[:, :LAT])
        accum = accum + jnp.einsum('sdhu,udc->sdhc', new_w.astype(jnp.bfloat16).astype(jnp.float32), fresh[..., :LAT])
        heads_out = jnp.einsum('sdhc,hcv->sdhv', accum, absorb_value.astype(jnp.float32), precision=lax.Precision.HIGHEST)
        result = (heads_out / total[..., None]).astype(jnp.bfloat16)
        return result.reshape(STEPS, DOCS, H * VHEAD)
    order = assignment.astype(jnp.int32)
    queries = q_decode[:, order].reshape(STEPS, SPANS, DOCS, H, NOPE + ROPE).transpose(1, 0, 2, 3, 4)
    fresh_latent = new_latent[:, order].reshape(STEPS, SPANS, DOCS, LAT).transpose(1, 0, 2, 3)
    fresh_rope = new_rope[:, order].reshape(STEPS, SPANS, DOCS, ROPE).transpose(1, 0, 2, 3)
    results = lax.map(decode_span, (queries, fresh_latent, fresh_rope, kv_latent, key_rope, segment_ids))
    results = results.transpose(1, 0, 2, 3).reshape(STEPS, SEQS, H * VHEAD)
    decode_out = jnp.zeros((STEPS, SEQS, H * VHEAD), jnp.bfloat16).at[:, order].set(results)
    return (prefill_out, decode_out)
```

```python
import math

import jax
import jax.numpy as jnp
from jax import lax
from jax.experimental import pallas as pl
from jax.experimental.pallas import tpu as pltpu
from jax.sharding import PartitionSpec as P

H = 64
NOPE = 128
ROPE = 64
LAT = 512
VHEAD = 128
TOK = 128
DOCS = 16
STEPS = 2
NSEQ = 16
NSPAN = 8
WIDE = 640
AUG = 64
BIG = float(2.0**100)
EPS = 1e-06
SCALE = (NOPE + ROPE) ** (-0.5)
EXPC = SCALE * math.log2(math.e)
GROUP = 8
NG = H // GROUP
CH = 2
QCOL = 2048 + 2 * WIDE
BF = jnp.bfloat16
F32 = jnp.float32
MESH = pl.DeviceIdType.MESH


def cache_rows(latent, rope):
    values = latent.astype(F32)
    normed = values * lax.rsqrt(jnp.mean(values * values, axis=-1, keepdims=True) + EPS)
    return jnp.concatenate([normed, rope.astype(F32)], axis=-1).astype(BF)


def nt_dot(a, b):
    return lax.dot_general(a, b, (((1,), (1,)), ((), ())), preferred_element_type=F32)


def nn_dot(a, b):
    return jnp.dot(a, b, preferred_element_type=F32)


def kernel(
    own_ref, qm_ref, sel_ref, selo_ref, qaug_ref, daug_ref, faug_ref, tri_ref, wkd_ref, wvd_ref,
    q_ref, wk_ref, wv_ref,
    out_ref, dec_ref,
    cb, qa, qf, qr, qall, do_own, doall, so, outbuf,
    g_send, g_recv, q_send, q_recv, o_send, o_recv, s_send, s_recv,
):
    step = pl.program_id(0)
    me = lax.axis_index("seq")
    span = lax.axis_index("span")
    z = me // 4
    yh = (me // 2) % 2
    k = me % 2
    zp = (z + 1) % 4
    zm = (z + 3) % 4
    z2 = (z + 2) % 4

    def idx(zz, yy, kk):
        return zz * 4 + yy * 2 + kk

    part = idx(z, yh, 1 - k)
    ypeer = idx(z, 1 - yh, k)
    up = idx(zp, yh, k)
    down = idx(zm, yh, k)

    def rows(block, owner):
        slot = (block - owner + 24) % 16
        return cb.at[pl.ds(pl.multiple_of(slot * TOK, TOK), TOK)]

    kinds = [
        idx(z, 1 - yh, k),
        idx(zm, yh, k),
        idx(zp, yh, k),
        idx(zm, 1 - yh, k),
        idx(zp, 1 - yh, k),
        idx(z2, yh, k),
        idx(z2, 1 - yh, k),
    ]
    arrive = kinds + [part] + [b + 1 - 2 * k for b in kinds]

    def copy(src, block, target, kind, send, dst=None):
        return pltpu.make_async_remote_copy(
            src_ref=src,
            dst_ref=rows(block, target) if dst is None else dst,
            send_sem=g_send.at[send],
            recv_sem=g_recv.at[kind],
            device_id=(target, span),
            device_id_type=MESH,
        )

    plan = [
        (None, me, ypeer, 0),
        (None, me, up, 1),
        (None, me, part, 7),
        (None, me, down, 2),
        (0, kinds[0], up, 3),
        (0, kinds[0], down, 4),
        (0, kinds[0], part, 8),
        (1, kinds[1], up, 5),
        (1, kinds[1], part, 9),
        (3, kinds[3], part, 11),
        (4, kinds[4], down, 6),
        (4, kinds[4], part, 12),
        (2, kinds[2], part, 10),
        (5, kinds[5], part, 13),
        (6, kinds[6], part, 14),
    ]

    def send(i):
        source, block, target, kind = plan[i]
        src = own_ref if source is None else rows(block, me)
        return copy(src, block, target, kind, i)

    def landed(kind):
        copy(own_ref, arrive[kind], part, kind, 0, rows(arrive[kind], me)).wait_recv()

    def q_copy(off):
        return pltpu.make_async_remote_copy(
            src_ref=qm_ref,
            dst_ref=qall.at[pl.ds(pl.multiple_of(span * DOCS, DOCS), DOCS)],
            send_sem=q_send.at[off - 1],
            recv_sem=q_recv.at[off - 1],
            device_id=(me, (span + off) % NSPAN),
            device_id_type=MESH,
        )

    def o_copy(off):
        return pltpu.make_async_remote_copy(
            src_ref=do_own,
            dst_ref=doall.at[span],
            send_sem=o_send.at[off - 1],
            recv_sem=o_recv.at[off - 1],
            device_id=(me, (span + off) % NSPAN),
            device_id_type=MESH,
        )

    def s_copy(off):
        return pltpu.make_async_remote_copy(
            src_ref=so,
            dst_ref=outbuf.at[:, :, pl.ds(pl.multiple_of(me * 512, 512), 512)],
            send_sem=s_send.at[off - 1],
            recv_sem=s_recv.at[off - 1],
            device_id=((me + off) % NSEQ, span),
            device_id_type=MESH,
        )

    @pl.when(step == 0)
    def _():
        barrier = pltpu.get_barrier_semaphore()
        for off in range(1, NSEQ):
            pl.semaphore_signal(
                barrier, inc=1, device_id=((me + off) % NSEQ, span), device_id_type=MESH
            )
        for off in range(1, NSPAN):
            pl.semaphore_signal(
                barrier, inc=1, device_id=(me, (span + off) % NSPAN), device_id_type=MESH
            )
        pl.semaphore_wait(barrier, NSEQ + NSPAN - 2)
        for i in range(4):
            send(i).start()
        for off in (1, 7, 2, 6, 3, 5, 4):
            q_copy(off).start()
        cb[pl.ds(8 * TOK, TOK), :] = own_ref[...]
        qall[pl.ds(pl.multiple_of(span * DOCS, DOCS), DOCS), :] = qm_ref[...]

    @pl.when(step < NG)
    def _():
        block = q_ref[...].astype(F32).reshape(TOK * GROUP, NOPE + ROPE)
        qf[...] = block[:, 0:NOPE]
        qr[:, 0:ROPE] = block[:, NOPE:]
        for j in range(GROUP):
            nope = qf[pl.ds(j, TOK, stride=GROUP), :].astype(BF)
            rope = qr[pl.ds(j, TOK, stride=GROUP), :][:, 0:ROPE].astype(BF)
            at = pl.ds(pl.multiple_of((step * GROUP + j) * TOK, TOK), TOK)
            qa[at, 0:LAT] = nn_dot(nope, wk_ref[j]).astype(BF)
            qa[at, LAT:WIDE] = jnp.concatenate([rope, qaug_ref[...]], axis=1)

    @pl.when(step == NG)
    def _():
        landed(1)
        send(7).start()
        send(8).start()
        landed(0)
        for i in (4, 5, 6):
            send(i).start()
        landed(3)
        send(9).start()
        landed(4)
        send(10).start()
        send(11).start()
        landed(2)
        send(12).start()
        landed(5)
        send(13).start()
        landed(6)
        send(14).start()
        for kind in range(7, 15):
            landed(kind)
        for i in range(15):
            send(i).wait_send()

    @pl.when(step >= NG)
    def _():
        base = (step - NG) * GROUP * TOK
        keys = cb[pl.ds(0, 9 * TOK), :]
        vals = cb[pl.ds(0, 9 * TOK), pl.ds(0, LAT)]
        tri = jnp.concatenate([tri_ref[...]] * CH, axis=0)
        count = GROUP // CH

        def score(n):
            at = pl.ds(pl.multiple_of(base + n * CH * TOK, CH * TOK), CH * TOK)
            return nt_dot(qa[at, :], keys)

        s_next = score(0)
        for n in range(count):
            s = s_next
            if n + 1 < count:
                s_next = score(n + 1)
            s = jnp.concatenate([s[:, : 8 * TOK], s[:, 8 * TOK :] + tri], axis=1)
            best = jnp.max(s, axis=1, keepdims=True)
            w = jnp.exp2((s - best) * EXPC)
            total = jnp.sum(w, axis=1, keepdims=True)
            o = (nn_dot(w.astype(BF), vals) / total).astype(BF)
            for j in range(CH):
                h = n * CH + j
                out_ref[:, h * VHEAD : (h + 1) * VHEAD] = nn_dot(
                    o[j * TOK : (j + 1) * TOK], wv_ref[h]
                ).astype(BF)

    @pl.when(step == NG + 1)
    def _():
        for off in range(1, NSPAN):
            q_copy(off).wait()
        chosen = nn_dot(sel_ref[...], qall[...]).astype(BF)
        fresh = [
            chosen[:, 2048 + u * WIDE : 2048 + (u + 1) * WIDE] + faug_ref[pl.ds(u * DOCS, DOCS), :]
            for u in range(STEPS)
        ]
        cb[pl.ds(16 * TOK, TOK), :] = jnp.concatenate(
            fresh + [faug_ref[pl.ds(STEPS * DOCS, TOK - STEPS * DOCS), :]], axis=0
        )
        parts = []
        for j in range(4):
            nope = jnp.concatenate(
                [chosen[:, (j * 2 + t) * 256 : (j * 2 + t) * 256 + 128] for t in range(STEPS)], axis=0
            )
            rope = jnp.concatenate(
                [chosen[:, (j * 2 + t) * 256 + 128 : (j * 2 + t + 1) * 256] for t in range(STEPS)],
                axis=0,
            )
            lat = nn_dot(nope, wkd_ref[j]).astype(BF)
            parts.append(jnp.concatenate([lat, rope + daug_ref[...]], axis=1))
        dq = jnp.concatenate(parts, axis=0)
        s = nt_dot(dq, cb[...])
        best = jnp.max(s, axis=1, keepdims=True)
        w = jnp.exp2((s - best) * EXPC)
        total = jnp.sum(w, axis=1, keepdims=True)
        acc = nn_dot(w.astype(BF), cb[:, pl.ds(0, LAT)])
        for j in range(4):
            rest = acc[j * 32 : (j + 1) * 32]
            split = []
            for _ in range(3):
                piece = rest.astype(BF)
                split.append(piece)
                rest = rest - piece.astype(F32)
            y = nn_dot(jnp.concatenate(split, axis=0), wvd_ref[j])
            y = (y[0:32] + y[32:64] + y[64:96]) / total[j * 32 : (j + 1) * 32]
            y = y.astype(BF)
            for t in range(STEPS):
                do_own[t, :, j * VHEAD : (j + 1) * VHEAD] = y[t * DOCS : (t + 1) * DOCS]

    @pl.when(step == NG + 2)
    def _():
        for off in (1, 7, 2, 6, 3, 5, 4):
            o_copy(off).start()
        doall[span] = do_own[...]

    @pl.when(step == NG + 4)
    def _():
        for off in range(1, NSPAN):
            o_copy(off).wait()
        for t in range(STEPS):
            full = jnp.concatenate([doall[i, t] for i in range(NSPAN)], axis=0)
            so[t] = nn_dot(selo_ref[...], full).astype(BF)

    @pl.when(step == NG + 5)
    def _():
        for off in range(1, NSEQ):
            s_copy(off).start()
        outbuf[:, :, pl.ds(pl.multiple_of(me * 512, 512), 512)] = so[...]

    @pl.when(step == 2 * NG - 1)
    def _():
        for off in range(1, NSEQ):
            s_copy(off).wait()
        dec_ref[...] = outbuf[...]


def body(
    q_prefill, kv_latent, key_rope, segment_ids, assignment, absorb_key, absorb_value,
    q_decode, new_latent, new_rope,
):
    me = lax.axis_index("seq")
    span = lax.axis_index("span")
    seg = lax.dynamic_slice(segment_ids, (span, me * TOK), (1, TOK))[0]
    numbers = jnp.arange(DOCS, dtype=jnp.int32)
    same = seg[:, None] == numbers[None, :]
    here = jnp.broadcast_to((numbers == me)[None, :], (TOK, NSEQ))
    zeros32 = jnp.zeros((TOK, AUG - 32), F32)
    own_aug = jnp.concatenate([same.astype(F32), here.astype(F32), zeros32], axis=1).astype(BF)
    own = jnp.concatenate([cache_rows(kv_latent[0], key_rope[0]), own_aug], axis=1)
    later = jnp.broadcast_to((numbers > me)[None, :], (TOK, NSEQ))
    qaug = jnp.concatenate(
        [jnp.where(same, 0.0, -BIG), jnp.where(later, -BIG, 0.0), zeros32], axis=1
    ).astype(BF)

    mine = lax.dynamic_slice(q_decode, (0, 0, me * 4, 0), (STEPS, DOCS, 4, NOPE + ROPE))
    mine = jnp.pad(mine, ((0, 0), (0, 0), (0, 0), (0, 64))).transpose(1, 2, 0, 3).reshape(DOCS, 2048)
    fresh = jnp.pad(cache_rows(new_latent, new_rope), ((0, 0), (0, 0), (0, AUG)))
    qm = jnp.concatenate([mine, fresh[0], fresh[1]], axis=1)

    every = jnp.arange(NSPAN * DOCS, dtype=jnp.int32)
    own_docs = lax.dynamic_slice(assignment, (span * DOCS,), (DOCS,))
    sel = (own_docs[:, None] == every[None, :]).astype(BF)
    selo = (assignment[None, :] == (span * DOCS + numbers)[:, None]).astype(BF)

    row = jnp.arange(STEPS * DOCS, dtype=jnp.int32)
    col = jnp.arange(128, dtype=jnp.int32) - ROPE
    not_doc = (col[None, :] >= 0) & (col[None, :] < 16) & (col[None, :] != (row % DOCS)[:, None])
    not_step = (col[None, :] == 32) & ((row // DOCS)[:, None] == 0)
    daug = jnp.where(not_doc | not_step | (col == 33)[None, :], -BIG, 0.0).astype(BF)
    frow = jnp.arange(TOK, dtype=jnp.int32)
    fcol = jnp.arange(WIDE, dtype=jnp.int32) - LAT - ROPE
    real = (frow < STEPS * DOCS)[:, None]
    fdoc = real & (fcol[None, :] >= 0) & (fcol[None, :] < 16) & (fcol[None, :] == (frow % DOCS)[:, None])
    fstep = real & (fcol == 32)[None, :] & ((frow // DOCS) == 1)[:, None]
    fpad = (~real) & (fcol == 33)[None, :]
    faug = (fdoc | fstep | fpad).astype(BF)
    tri = jnp.where(frow[:, None] >= frow[None, :], 0.0, -1e30).astype(F32)

    wkd = lax.dynamic_slice(absorb_key, (me * 4, 0, 0), (4, NOPE, LAT))
    wvd = lax.dynamic_slice(absorb_value, (me * 4, 0, 0), (4, LAT, VHEAD))

    vmem = pl.BlockSpec(memory_space=pltpu.VMEM)
    out, dec = pl.pallas_call(
        kernel,
        grid=(2 * NG,),
        out_shape=(
            jax.ShapeDtypeStruct((TOK, H * VHEAD), BF),
            jax.ShapeDtypeStruct((STEPS, DOCS, H * VHEAD), BF),
        ),
        in_specs=[vmem] * 10
        + [
            pl.BlockSpec((TOK, GROUP, NOPE + ROPE), lambda i: (0, jnp.minimum(i, NG - 1), 0)),
            pl.BlockSpec((GROUP, NOPE, LAT), lambda i: (jnp.minimum(i, NG - 1), 0, 0)),
            pl.BlockSpec((GROUP, LAT, VHEAD), lambda i: (jnp.maximum(i - NG, 0), 0, 0)),
        ],
        out_specs=(
            pl.BlockSpec((TOK, GROUP * VHEAD), lambda i: (0, jnp.maximum(i - NG, 0))),
            pl.BlockSpec((STEPS, DOCS, H * VHEAD), lambda i: (0, 0, 0)),
        ),
        scratch_shapes=[
            pltpu.VMEM((17 * TOK, WIDE), BF),
            pltpu.VMEM((H * TOK, WIDE), BF),
            pltpu.VMEM((TOK * GROUP, NOPE), F32),
            pltpu.VMEM((TOK * GROUP, NOPE), F32),
            pltpu.VMEM((NSPAN * DOCS, QCOL), BF),
            pltpu.VMEM((STEPS, DOCS, 512), BF),
            pltpu.VMEM((NSPAN, STEPS, DOCS, 512), BF),
            pltpu.VMEM((STEPS, DOCS, 512), BF),
            pltpu.VMEM((STEPS, DOCS, H * VHEAD), BF),
            pltpu.SemaphoreType.DMA((15,)),
            pltpu.SemaphoreType.DMA((15,)),
            pltpu.SemaphoreType.DMA((7,)),
            pltpu.SemaphoreType.DMA((7,)),
            pltpu.SemaphoreType.DMA((7,)),
            pltpu.SemaphoreType.DMA((7,)),
            pltpu.SemaphoreType.DMA((15,)),
            pltpu.SemaphoreType.DMA((15,)),
        ],
        compiler_params=pltpu.CompilerParams(
            dimension_semantics=("arbitrary",),
            collective_id=0,
            has_side_effects=True,
            vmem_limit_bytes=60 * 1024 * 1024,
        ),
    )(
        own, qm, sel, selo, qaug, daug, faug, tri, wkd, wvd,
        q_prefill[0], absorb_key, absorb_value,
    )
    return (out[None], dec)


def solution(mesh):
    in_specs = (
        P("span", "seq", None, None),
        P("span", "seq", None),
        P("span", "seq", None),
        P(),
        P(),
        P(),
        P(),
        P(None, "span", None, None),
        P(None, "span", None),
        P(None, "span", None),
    )
    out_specs = (P("span", "seq", None), P(None, "span", None))
    return jax.shard_map(body, mesh=mesh, in_specs=in_specs, out_specs=out_specs, check_vma=False)
```

```python
import math

import jax
import jax.numpy as jnp
from jax import lax
from jax.experimental import pallas as pl
from jax.experimental.pallas import tpu as pltpu
from jax.sharding import PartitionSpec as P

H = 64
NOPE = 128
ROPE = 64
LAT = 512
VHEAD = 128
TOK = 128
DOCS = 16
STEPS = 2
NSEQ = 16
NSPAN = 8
WIDE = 640
AUG = 64
BIG = float(2.0**100)
EPS = 1e-06
SCALE = (NOPE + ROPE) ** (-0.5)
EXPC = SCALE * math.log2(math.e)
GROUP = 8
NG = H // GROUP
CH = 2
RELAY0 = 4
RELAY1 = 6
DEC = NG + 2
QCOL = 2688
FRESH = 1536
BF = jnp.bfloat16
F32 = jnp.float32
MESH = pl.DeviceIdType.MESH


def normed(values):
    values = values.astype(F32)
    mean = jnp.mean(values * values, axis=-1, keepdims=True)
    return values * lax.rsqrt(mean + EPS)


def iota(shape, dim):
    return lax.broadcasted_iota(jnp.int32, shape, dim)


def nt_dot(a, b):
    return lax.dot_general(a, b, (((1,), (1,)), ((), ())), preferred_element_type=F32)


def nn_dot(a, b):
    return jnp.dot(a, b, preferred_element_type=F32)


def kernel(
    lat_ref, rope_ref, seg_ref, assign_ref, qd_ref, nl_ref, nr_ref, wk_any, wv_any,
    q_ref, wk_ref, wv_ref,
    out_ref, dec_ref,
    cb, qa, s1, qaug, qf, qr, qm, qall, selbuf, wkd, wvd, do_own, doall, so, outbuf,
    g_send, g_recv, q_send, q_recv, o_send, o_recv, s_send, s_recv, w_sem,
):
    step = pl.program_id(0)
    me = lax.axis_index("seq")
    span = lax.axis_index("span")
    z = me // 4
    yh = (me // 2) % 2
    k = me % 2
    zp = (z + 1) % 4
    zm = (z + 3) % 4
    z2 = (z + 2) % 4

    def idx(zz, yy, kk):
        return zz * 4 + yy * 2 + kk

    part = idx(z, yh, 1 - k)
    ypeer = idx(z, 1 - yh, k)
    up = idx(zp, yh, k)
    down = idx(zm, yh, k)

    def rows(block, owner):
        slot = (block - owner + 24) % 16
        return cb.at[pl.ds(pl.multiple_of(slot * TOK, TOK), TOK)]

    kinds = [
        idx(z, 1 - yh, k),
        idx(zm, yh, k),
        idx(zp, yh, k),
        idx(zm, 1 - yh, k),
        idx(zp, 1 - yh, k),
        idx(z2, yh, k),
        idx(z2, 1 - yh, k),
    ]
    arrive = kinds + [part] + [b + 1 - 2 * k for b in kinds]

    def copy(src, dst, target, kind, number):
        return pltpu.make_async_remote_copy(
            src_ref=src,
            dst_ref=dst,
            send_sem=g_send.at[number],
            recv_sem=g_recv.at[kind],
            device_id=(target, span),
            device_id_type=MESH,
        )

    plan = [
        (me, ypeer, 0),
        (me, up, 1),
        (me, part, 7),
        (me, down, 2),
        (kinds[0], up, 3),
        (kinds[0], down, 4),
        (kinds[0], part, 8),
        (kinds[1], up, 5),
        (kinds[1], part, 9),
        (kinds[3], part, 11),
        (kinds[4], down, 6),
        (kinds[4], part, 12),
        (kinds[2], part, 10),
        (kinds[5], part, 13),
        (kinds[6], part, 14),
    ]

    def send(i):
        block, target, kind = plan[i]
        return copy(rows(block, me), rows(block, target), target, kind, i)

    def landed(kind):
        dst = rows(arrive[kind], me)
        copy(dst, dst, part, kind, 0).wait_recv()

    x = span // 2
    lo = span % 2
    lopeer = x * 2 + 1 - lo

    def qrows(src):
        return qall.at[pl.ds(pl.multiple_of(src * DOCS, DOCS), DOCS)]

    def q_copy(src, dst, target, number):
        return pltpu.make_async_remote_copy(
            src_ref=src,
            dst_ref=dst,
            send_sem=q_send.at[number],
            recv_sem=q_recv.at[number],
            device_id=(me, target),
            device_id_type=MESH,
        )

    def q_send_of(number):
        if number == 0:
            return q_copy(qm, qrows(span), lopeer, 0)
        xx = (x + (number - 1) % 3 + 1) % 4
        if number <= 3:
            return q_copy(qm, qrows(span), xx * 2 + lo, number)
        return q_copy(qrows(lopeer), qrows(lopeer), xx * 2 + lo, number)

    def q_landed(number):
        if number == 0:
            src = lopeer
        else:
            xx = (x + 3 - (number - 1) % 3) % 4
            src = xx * 2 + (lo if number <= 3 else 1 - lo)
        q_copy(qrows(src), qrows(src), lopeer, number).wait_recv()

    def o_copy(off):
        return pltpu.make_async_remote_copy(
            src_ref=do_own,
            dst_ref=doall.at[span],
            send_sem=o_send.at[off - 1],
            recv_sem=o_recv.at[off - 1],
            device_id=(me, (span + off) % NSPAN),
            device_id_type=MESH,
        )

    def columns(block):
        return outbuf.at[:, :, pl.ds(pl.multiple_of(block * 512, 512), 512)]

    def s_copy(src, dst, target, number):
        return pltpu.make_async_remote_copy(
            src_ref=src,
            dst_ref=dst,
            send_sem=s_send.at[number],
            recv_sem=s_recv.at[number],
            device_id=(target, span),
            device_id_type=MESH,
        )

    def chip(off):
        return ((me // 2 + off) % 8) * 2 + k

    def s_out(number):
        if number == 7:
            return s_copy(so, columns(me), part, 7)
        if number < 7:
            return s_copy(so, columns(me), chip(number + 1), number)
        block = chip(8 - (number - 7))
        return s_copy(columns(block), columns(block), part, number)

    def s_landed(number):
        if number == 7:
            block = part
        elif number < 7:
            block = chip(8 - (number + 1))
        else:
            block = chip(8 - (number - 7)) + 1 - 2 * k
        s_copy(columns(block), columns(block), part, number).wait_recv()

    wk_copy = lambda: pltpu.make_async_copy(wk_any.at[pl.ds(me * 4, 4)], wkd, w_sem.at[0])
    wv_copy = lambda: pltpu.make_async_copy(wv_any.at[pl.ds(me * 4, 4)], wvd, w_sem.at[1])

    @pl.when(step == 0)
    def _():
        barrier = pltpu.get_barrier_semaphore()
        for off in range(1, NSEQ):
            pl.semaphore_signal(
                barrier, inc=1, device_id=((me + off) % NSEQ, span), device_id_type=MESH
            )
        for off in range(1, NSPAN):
            pl.semaphore_signal(
                barrier, inc=1, device_id=(me, (span + off) % NSPAN), device_id_type=MESH
            )
        wk_copy().start()
        wv_copy().start()
        cb[pl.ds(8 * TOK, TOK), 0:LAT] = normed(lat_ref[...]).astype(BF)
        segs = seg_ref[:, pl.ds(pl.multiple_of(me * TOK, TOK), TOK)].astype(F32)
        seg = jnp.sum(jnp.where(iota((NSPAN, TOK), 0) == span, segs, 0.0), axis=0, keepdims=True)
        seg = seg.astype(jnp.int32)
        number = iota((AUG, TOK), 0)
        same = number == seg
        kaug = jnp.where(same | (number - 16 == me), 1.0, 0.0)
        late = (number >= 16) & (number < 32) & (number - 16 > me)
        wrong = ((number < 16) & jnp.logical_not(same)) | late
        qaug[...] = jnp.where(wrong, -BIG, 0.0).astype(BF)
        tail = jnp.concatenate([rope_ref[...].astype(F32), kaug], axis=0)
        cb[pl.ds(8 * TOK, TOK), LAT:WIDE] = tail.T.astype(BF)
        at8 = pl.ds(pl.multiple_of((me // 2) * 8, 8), 8)
        for t in range(STEPS):
            block = qd_ref[t, :, at8, :].astype(F32).reshape(DOCS * 8, NOPE + ROPE)
            qf[t] = block[:, 0:NOPE]
            qr[t, :, 0:ROPE] = block[:, NOPE:]
        for j in range(4):
            ropes = []
            for t in range(STEPS):
                pick = pl.ds(k * 4 + j, DOCS, stride=8)
                n = j * 2 + t
                qm[:, n * 128 : (n + 1) * 128] = qf.at[t][pick, :].astype(BF)
                ropes.append(qr.at[t][pick, :][:, 0:ROPE])
            qm[:, 1024 + j * 128 : 1024 + (j + 1) * 128] = jnp.concatenate(ropes, axis=1).astype(BF)
        for t in range(STEPS):
            qm[:, FRESH + t * LAT : FRESH + (t + 1) * LAT] = normed(nl_ref[t]).astype(BF)
        both = jnp.concatenate([nr_ref[0].astype(F32), nr_ref[1].astype(F32)], axis=1)
        qm[:, FRESH + 2 * LAT : QCOL] = both.astype(BF)
        pl.semaphore_wait(barrier, NSEQ + NSPAN - 2)
        for i in (1, 0, 2):
            send(i).start()
        for n in (1, 3, 2):
            q_send_of(n).start()
        qrows(span)[...] = qm[...]
        selbuf[...] = jnp.where(assign_ref[...] == iota((128, 128), 0), 1.0, 0.0).T

    @pl.when(step < NG)
    def _():
        own_keys = cb[pl.ds(8 * TOK, TOK), :]
        tri = jnp.where(iota((TOK, TOK), 0) >= iota((TOK, TOK), 1), 0.0, -1e30)
        first = pl.multiple_of(step * GROUP * TOK, GROUP * TOK)
        for j in range(GROUP):
            at = pl.ds(pl.multiple_of(first + j * TOK, TOK), TOK)
            nope = q_ref[j, 0:NOPE, :].T
            qa[at, 0:LAT] = nn_dot(nope, wk_ref[j]).astype(BF)
            qa[at, LAT:WIDE] = jnp.concatenate([q_ref[j, NOPE:, :], qaug[...]], axis=0).T
        for j in range(0, GROUP, 4):
            at = pl.ds(pl.multiple_of(first + j * TOK, 4 * TOK), 4 * TOK)
            s1[at, :] = nt_dot(qa[at, :], own_keys) + jnp.concatenate([tri] * 4, axis=0)

    @pl.when(step == RELAY0)
    def _():
        landed(1)
        send(7).start()
        send(8).start()

    @pl.when(step == RELAY1)
    def _():
        landed(0)
        for i in (4, 5, 6, 3):
            send(i).start()
        q_send_of(0).start()

    @pl.when(step == NG)
    def _():
        landed(3)
        send(9).start()
        landed(4)
        send(10).start()
        send(11).start()
        landed(5)
        send(13).start()
        landed(6)
        send(14).start()
        q_landed(0)
        for n in (4, 6, 5):
            q_send_of(n).start()
        for kind in (7, 8, 9, 11, 13, 14):
            landed(kind)

    @pl.when(step == NG + 1)
    def _():
        landed(2)
        send(12).start()

    @pl.when(step == DEC)
    def _():
        landed(10)
        landed(12)
        for i in range(15):
            send(i).wait_send()
        wk_copy().wait()
        wv_copy().wait()
        for n in range(1, 7):
            q_landed(n)
        for n in range(7):
            q_send_of(n).wait_send()
        sel = selbuf[pl.ds(pl.multiple_of(span * DOCS, DOCS), DOCS), :].astype(BF)
        chosen = nn_dot(sel, qall[...]).astype(BF)
        col = iota((DOCS, AUG), 1)
        doc = iota((DOCS, AUG), 0)
        last = FRESH + 2 * LAT
        for t in range(STEPS):
            at = pl.ds(16 * TOK + t * DOCS, DOCS)
            cb[at, 0:LAT] = chosen[:, FRESH + t * LAT : FRESH + (t + 1) * LAT]
            mark = jnp.where((col == doc) | ((col == 32) & (t == 1)), 1.0, 0.0)
            rope = chosen[:, last + t * ROPE : last + (t + 1) * ROPE].astype(F32)
            cb[at, LAT:WIDE] = jnp.concatenate([rope, mark], axis=1).astype(BF)
        pad = TOK - STEPS * DOCS
        cb[pl.ds(16 * TOK + STEPS * DOCS, pad), :] = jnp.where(
            iota((pad, WIDE), 1) == LAT + ROPE + 33, 1.0, 0.0
        ).astype(BF)
        row = iota((STEPS * DOCS, AUG), 0)
        dcol = iota((STEPS * DOCS, AUG), 1)
        wrong = ((dcol < 16) & (dcol != row % DOCS)) | ((dcol == 32) & (row < DOCS)) | (dcol == 33)
        daug = jnp.where(wrong, -BIG, 0.0)
        parts = []
        for j in range(4):
            nope = jnp.concatenate(
                [chosen[:, (j * 2 + t) * 128 : (j * 2 + t + 1) * 128] for t in range(STEPS)], axis=0
            )
            at = 1024 + j * 128
            rope = jnp.concatenate(
                [chosen[:, at + t * ROPE : at + (t + 1) * ROPE] for t in range(STEPS)], axis=0
            )
            lat = nn_dot(nope, wkd[j]).astype(BF)
            end = jnp.concatenate([rope.astype(F32), daug], axis=1).astype(BF)
            parts.append(jnp.concatenate([lat, end], axis=1))
        dq = jnp.concatenate(parts, axis=0)
        s = nt_dot(dq, cb[...])
        best = jnp.max(s, axis=1, keepdims=True)
        w = jnp.exp2((s - best) * EXPC)
        total = jnp.sum(w, axis=1, keepdims=True)
        acc = nn_dot(w.astype(BF), cb[:, pl.ds(0, LAT)])
        for j in range(4):
            rest = acc[j * 32 : (j + 1) * 32]
            split = []
            for _ in range(3):
                piece = rest.astype(BF)
                split.append(piece)
                rest = rest - piece.astype(F32)
            y = nn_dot(jnp.concatenate(split, axis=0), wvd[j])
            y = (y[0:32] + y[32:64] + y[64:96]) / total[j * 32 : (j + 1) * 32]
            y = y.astype(BF)
            for t in range(STEPS):
                do_own[t, :, j * VHEAD : (j + 1) * VHEAD] = y[t * DOCS : (t + 1) * DOCS]

    @pl.when(step == DEC + 2)
    def _():
        for off in range(1, NSPAN):
            o_copy(off).wait()
        selo = jnp.where(assign_ref[...] == span * DOCS + iota((DOCS, 128), 0), 1.0, 0.0).astype(BF)
        for t in range(STEPS):
            full = jnp.concatenate([doall[i, t] for i in range(NSPAN)], axis=0)
            so[t] = nn_dot(selo, full).astype(BF)

    @pl.when(step >= NG)
    def _():
        base = (step - NG) * GROUP * TOK
        count = GROUP // CH

        def at(n):
            return pl.ds(pl.multiple_of(base + n * CH * TOK, CH * TOK), CH * TOK)

        def score(n):
            return nt_dot(qa[at(n), :], cb[pl.ds(0, 8 * TOK), :])

        s_next = score(0)
        for n in range(count):
            s = s_next
            if n + 1 < count:
                s_next = score(n + 1)
            s = jnp.concatenate([s, s1[at(n), :]], axis=1)
            best = jnp.max(s, axis=1, keepdims=True)
            w = jnp.exp2((s - best) * EXPC)
            total = jnp.sum(w, axis=1, keepdims=True)
            o = (nn_dot(w.astype(BF), cb[pl.ds(0, 9 * TOK), pl.ds(0, LAT)]) / total).astype(BF)
            for j in range(CH):
                h = n * CH + j
                out_ref[:, h * VHEAD : (h + 1) * VHEAD] = nn_dot(
                    o[j * TOK : (j + 1) * TOK], wv_ref[h]
                ).astype(BF)

    @pl.when(step == DEC)
    def _():
        for off in (1, 7, 2, 6, 3, 5, 4):
            o_copy(off).start()
        doall[span] = do_own[...]

    @pl.when(step == DEC + 2)
    def _():
        for n in (3, 0, 6, 1, 5, 2, 4, 7):
            s_out(n).start()
        columns(me)[...] = so[...]

    @pl.when(step == 2 * NG - 1)
    def _():
        for n in range(7):
            s_landed(n)
            s_out(8 + n).start()
        for n in range(7, 15):
            s_landed(n)
        for n in range(15):
            s_out(n).wait_send()
        dec_ref[...] = outbuf[...]


def body(
    q_prefill, kv_latent, key_rope, segment_ids, assignment, absorb_key, absorb_value,
    q_decode, new_latent, new_rope,
):
    vmem = pl.BlockSpec(memory_space=pltpu.VMEM)
    hbm = pl.BlockSpec(memory_space=pl.ANY)
    out, dec = pl.pallas_call(
        kernel,
        grid=(2 * NG,),
        out_shape=(
            jax.ShapeDtypeStruct((TOK, H * VHEAD), BF),
            jax.ShapeDtypeStruct((STEPS, DOCS, H * VHEAD), BF),
        ),
        in_specs=[vmem] * 7
        + [
            hbm,
            hbm,
            pl.BlockSpec((GROUP, NOPE + ROPE, TOK), lambda i: (jnp.minimum(i, NG - 1), 0, 0)),
            pl.BlockSpec((GROUP, NOPE, LAT), lambda i: (jnp.minimum(i, NG - 1), 0, 0)),
            pl.BlockSpec((GROUP, LAT, VHEAD), lambda i: (jnp.maximum(i - NG, 0), 0, 0)),
        ],
        out_specs=(
            pl.BlockSpec((TOK, GROUP * VHEAD), lambda i: (0, jnp.maximum(i - NG, 0))),
            pl.BlockSpec((STEPS, DOCS, H * VHEAD), lambda i: (0, 0, 0)),
        ),
        scratch_shapes=[
            pltpu.VMEM((17 * TOK, WIDE), BF),
            pltpu.VMEM((H * TOK, WIDE), BF),
            pltpu.VMEM((H * TOK, TOK), F32),
            pltpu.VMEM((AUG, TOK), BF),
            pltpu.VMEM((STEPS, DOCS * 8, NOPE), F32),
            pltpu.VMEM((STEPS, DOCS * 8, NOPE), F32),
            pltpu.VMEM((DOCS, QCOL), BF),
            pltpu.VMEM((NSPAN * DOCS, QCOL), BF),
            pltpu.VMEM((128, 128), F32),
            pltpu.VMEM((4, NOPE, LAT), BF),
            pltpu.VMEM((4, LAT, VHEAD), BF),
            pltpu.VMEM((STEPS, DOCS, 512), BF),
            pltpu.VMEM((NSPAN, STEPS, DOCS, 512), BF),
            pltpu.VMEM((STEPS, DOCS, 512), BF),
            pltpu.VMEM((STEPS, DOCS, H * VHEAD), BF),
            pltpu.SemaphoreType.DMA((15,)),
            pltpu.SemaphoreType.DMA((15,)),
            pltpu.SemaphoreType.DMA((7,)),
            pltpu.SemaphoreType.DMA((7,)),
            pltpu.SemaphoreType.DMA((7,)),
            pltpu.SemaphoreType.DMA((7,)),
            pltpu.SemaphoreType.DMA((15,)),
            pltpu.SemaphoreType.DMA((15,)),
            pltpu.SemaphoreType.DMA((2,)),
        ],
        compiler_params=pltpu.CompilerParams(
            dimension_semantics=("arbitrary",),
            collective_id=0,
            has_side_effects=True,
            vmem_limit_bytes=60 * 1024 * 1024,
        ),
    )(
        kv_latent[0], key_rope[0].T, segment_ids, assignment.reshape(1, 128), q_decode,
        new_latent, new_rope, absorb_key, absorb_value,
        q_prefill[0].transpose(1, 2, 0), absorb_key, absorb_value,
    )
    return (out[None], dec)


def solution(mesh):
    in_specs = (
        P("span", "seq", None, None),
        P("span", "seq", None),
        P("span", "seq", None),
        P(),
        P(),
        P(),
        P(),
        P(None, "span", None, None),
        P(None, "span", None),
        P(None, "span", None),
    )
    out_specs = (P("span", "seq", None), P(None, "span", None))
    return jax.shard_map(body, mesh=mesh, in_specs=in_specs, out_specs=out_specs, check_vma=False)
```

```python
import math

import jax
import jax.numpy as jnp
from jax import lax
from jax.experimental import pallas as pl
from jax.experimental.pallas import tpu as pltpu
from jax.sharding import PartitionSpec as P

H = 64
NOPE = 128
ROPE = 64
LAT = 512
VHEAD = 128
TOK = 128
DOCS = 16
STEPS = 2
NSEQ = 16
NSPAN = 8
WIDE = 640
AUG = 64
BIG = float(2.0**100)
EPS = 1e-06
SCALE = (NOPE + ROPE) ** (-0.5)
EXPC = SCALE * math.log2(math.e)
GROUP = 8
NG = H // GROUP
CH = 4
RELAY0 = 5
EARLY = NG
MIDDLE = NG + 1
LATE = NG + 2
DEC = LATE + 2
LAST = LATE + NG - 1
QCOL = 2688
FRESH = 1536
BF = jnp.bfloat16
F32 = jnp.float32
MESH = pl.DeviceIdType.MESH


def normed(values):
    values = values.astype(F32)
    mean = jnp.mean(values * values, axis=-1, keepdims=True)
    return values * lax.rsqrt(mean + EPS)


def iota(shape, dim):
    return lax.broadcasted_iota(jnp.int32, shape, dim)


def nt_dot(a, b):
    return lax.dot_general(a, b, (((1,), (1,)), ((), ())), preferred_element_type=F32)


def nn_dot(a, b):
    return jnp.dot(a, b, preferred_element_type=F32)


def kernel(
    lat_ref, rope_ref, seg_ref, assign_ref, qd_ref, nl_ref, nr_ref, wk_any, wv_any,
    q_ref, wk_ref, wv_ref,
    out_ref, dec_ref,
    cb, qa, s1, s2, s3, qaug, qf, qr, qm, qall, selbuf, wkd, wvd, do_own, doall, so, outbuf,
    g_send, g_recv, q_send, q_recv, o_send, o_recv, s_send, s_recv, w_sem,
):
    step = pl.program_id(0)
    me = lax.axis_index("seq")
    span = lax.axis_index("span")
    z = me // 4
    yh = (me // 2) % 2
    k = me % 2
    zp = (z + 1) % 4
    zm = (z + 3) % 4
    z2 = (z + 2) % 4

    def idx(zz, yy, kk):
        return zz * 4 + yy * 2 + kk

    part = idx(z, yh, 1 - k)
    ypeer = idx(z, 1 - yh, k)
    up = idx(zp, yh, k)
    down = idx(zm, yh, k)

    def less(a, b):
        return (b - a + 31) // 32

    def rows(block, owner):
        slot = (block - owner + 24) % 16
        phase = owner % 4
        back = (owner // 4 - block // 4 + 4) % 4
        near = less(0, back) * less(back, 2)
        other = (block % 4 // 2 + phase // 2) % 2
        high = less(7 - phase, slot) * less(slot, 8)
        place = near * (4 + 2 * other + block % 2) + (1 - near) * (slot - 4 * high)
        return cb.at[pl.ds(pl.multiple_of(place * TOK, TOK), TOK)]

    kinds = [
        idx(z, 1 - yh, k),
        idx(zm, yh, k),
        idx(zp, yh, k),
        idx(zm, 1 - yh, k),
        idx(zp, 1 - yh, k),
        idx(z2, yh, k),
        idx(z2, 1 - yh, k),
    ]
    arrive = kinds + [part] + [b + 1 - 2 * k for b in kinds]

    def copy(src, dst, target, kind, number):
        return pltpu.make_async_remote_copy(
            src_ref=src,
            dst_ref=dst,
            send_sem=g_send.at[number],
            recv_sem=g_recv.at[kind],
            device_id=(target, span),
            device_id_type=MESH,
        )

    plan = [
        (me, ypeer, 0),
        (me, up, 1),
        (me, part, 7),
        (me, down, 2),
        (kinds[0], up, 3),
        (kinds[0], down, 4),
        (kinds[0], part, 8),
        (kinds[1], up, 5),
        (kinds[1], part, 9),
        (kinds[3], part, 11),
        (kinds[4], down, 6),
        (kinds[4], part, 12),
        (kinds[2], part, 10),
        (kinds[5], part, 13),
        (kinds[6], part, 14),
    ]

    def send(i):
        block, target, kind = plan[i]
        return copy(rows(block, me), rows(block, target), target, kind, i)

    def landed(kind):
        dst = rows(arrive[kind], me)
        copy(dst, dst, part, kind, 0).wait_recv()

    x = span // 2
    lo = span % 2
    lopeer = x * 2 + 1 - lo

    def qrows(src):
        return qall.at[pl.ds(pl.multiple_of(src * DOCS, DOCS), DOCS)]

    def q_copy(src, dst, target, number):
        return pltpu.make_async_remote_copy(
            src_ref=src,
            dst_ref=dst,
            send_sem=q_send.at[number],
            recv_sem=q_recv.at[number],
            device_id=(me, target),
            device_id_type=MESH,
        )

    def q_send_of(number):
        if number == 0:
            return q_copy(qm, qrows(span), lopeer, 0)
        xx = (x + (number - 1) % 3 + 1) % 4
        if number <= 3:
            return q_copy(qm, qrows(span), xx * 2 + lo, number)
        return q_copy(qrows(lopeer), qrows(lopeer), xx * 2 + lo, number)

    def q_landed(number):
        if number == 0:
            src = lopeer
        else:
            xx = (x + 3 - (number - 1) % 3) % 4
            src = xx * 2 + (lo if number <= 3 else 1 - lo)
        q_copy(qrows(src), qrows(src), lopeer, number).wait_recv()

    def o_copy(off):
        return pltpu.make_async_remote_copy(
            src_ref=do_own,
            dst_ref=doall.at[span],
            send_sem=o_send.at[off - 1],
            recv_sem=o_recv.at[off - 1],
            device_id=(me, (span + off) % NSPAN),
            device_id_type=MESH,
        )

    def columns(block):
        return outbuf.at[:, :, pl.ds(pl.multiple_of(block * 512, 512), 512)]

    def s_copy(src, dst, target, number):
        return pltpu.make_async_remote_copy(
            src_ref=src,
            dst_ref=dst,
            send_sem=s_send.at[number],
            recv_sem=s_recv.at[number],
            device_id=(target, span),
            device_id_type=MESH,
        )

    def chip(off):
        return ((me // 2 + off) % 8) * 2 + k

    def s_out(number):
        if number == 7:
            return s_copy(so, columns(me), part, 7)
        if number < 7:
            return s_copy(so, columns(me), chip(number + 1), number)
        block = chip(8 - (number - 7))
        return s_copy(columns(block), columns(block), part, number)

    def s_landed(number):
        if number == 7:
            block = part
        elif number < 7:
            block = chip(8 - (number + 1))
        else:
            block = chip(8 - (number - 7)) + 1 - 2 * k
        s_copy(columns(block), columns(block), part, number).wait_recv()

    wk_copy = lambda: pltpu.make_async_copy(wk_any.at[pl.ds(me * 4, 4)], wkd, w_sem.at[0])
    wv_copy = lambda: pltpu.make_async_copy(wv_any.at[pl.ds(me * 4, 4)], wvd, w_sem.at[1])

    @pl.when(step == 0)
    def _():
        barrier = pltpu.get_barrier_semaphore()
        for off in range(1, NSEQ):
            pl.semaphore_signal(
                barrier, inc=1, device_id=((me + off) % NSEQ, span), device_id_type=MESH
            )
        for off in range(1, NSPAN):
            pl.semaphore_signal(
                barrier, inc=1, device_id=(me, (span + off) % NSPAN), device_id_type=MESH
            )
        wk_copy().start()
        wv_copy().start()
        cb[pl.ds(8 * TOK, TOK), 0:LAT] = normed(lat_ref[...]).astype(BF)
        segs = seg_ref[:, pl.ds(pl.multiple_of(me * TOK, TOK), TOK)].astype(F32)
        seg = jnp.sum(jnp.where(iota((NSPAN, TOK), 0) == span, segs, 0.0), axis=0, keepdims=True)
        seg = seg.astype(jnp.int32)
        number = iota((AUG, TOK), 0)
        same = number == seg
        kaug = jnp.where(same | (number - 16 == me), 1.0, 0.0)
        late = (number >= 16) & (number < 32) & (number - 16 > me)
        wrong = ((number < 16) & jnp.logical_not(same)) | late
        qaug[...] = jnp.where(wrong, -BIG, 0.0).astype(BF)
        tail = jnp.concatenate([rope_ref[...].astype(F32), kaug], axis=0)
        cb[pl.ds(8 * TOK, TOK), LAT:WIDE] = tail.T.astype(BF)
        at8 = pl.ds(pl.multiple_of((me // 2) * 8, 8), 8)
        for t in range(STEPS):
            block = qd_ref[t, :, at8, :].astype(F32).reshape(DOCS * 8, NOPE + ROPE)
            qf[t] = block[:, 0:NOPE]
            qr[t, :, 0:ROPE] = block[:, NOPE:]
        for j in range(4):
            ropes = []
            for t in range(STEPS):
                pick = pl.ds(k * 4 + j, DOCS, stride=8)
                n = j * 2 + t
                qm[:, n * 128 : (n + 1) * 128] = qf.at[t][pick, :].astype(BF)
                ropes.append(qr.at[t][pick, :][:, 0:ROPE])
            qm[:, 1024 + j * 128 : 1024 + (j + 1) * 128] = jnp.concatenate(ropes, axis=1).astype(BF)
        for t in range(STEPS):
            qm[:, FRESH + t * LAT : FRESH + (t + 1) * LAT] = normed(nl_ref[t]).astype(BF)
        both = jnp.concatenate([nr_ref[0].astype(F32), nr_ref[1].astype(F32)], axis=1)
        qm[:, FRESH + 2 * LAT : QCOL] = both.astype(BF)
        pl.semaphore_wait(barrier, NSEQ + NSPAN - 2)
        for i in (1, 0, 2):
            send(i).start()
        for n in (1, 3, 2):
            q_send_of(n).start()
        qrows(span)[...] = qm[...]
        selbuf[...] = jnp.where(assign_ref[...] == iota((128, 128), 0), 1.0, 0.0).T

    @pl.when(step < NG)
    def _():
        own_keys = cb[pl.ds(8 * TOK, TOK), :]
        tri = jnp.where(iota((TOK, TOK), 0) >= iota((TOK, TOK), 1), 0.0, -1e30)
        first = pl.multiple_of(step * GROUP * TOK, GROUP * TOK)
        for j in range(GROUP):
            at = pl.ds(pl.multiple_of(first + j * TOK, TOK), TOK)
            nope = q_ref[j, 0:NOPE, :].T
            qa[at, 0:LAT] = nn_dot(nope, wk_ref[j]).astype(BF)
            qa[at, LAT:WIDE] = jnp.concatenate([q_ref[j, NOPE:, :], qaug[...]], axis=0).T
        for j in range(0, GROUP, 4):
            at = pl.ds(pl.multiple_of(first + j * TOK, 4 * TOK), 4 * TOK)
            s1[at, :] = nt_dot(qa[at, :], own_keys) + jnp.concatenate([tri] * 4, axis=0)

    @pl.when(step == RELAY0)
    def _():
        landed(1)
        send(7).start()
        send(8).start()

    def early_scores(place, dst):
        keys = cb[pl.ds(place * TOK, 2 * TOK), :]

        def chunk(n, carry):
            at = pl.ds(pl.multiple_of(n * 4 * TOK, 4 * TOK), 4 * TOK)
            dst[at, :] = nt_dot(qa[at, :], keys)
            return carry

        lax.fori_loop(0, H // 4, chunk, 0)

    @pl.when(step == EARLY)
    def _():
        landed(0)
        for i in (4, 5, 6, 3):
            send(i).start()
        q_send_of(0).start()
        landed(9)
        early_scores(4, s2)

    @pl.when(step == MIDDLE)
    def _():
        landed(3)
        send(9).start()
        landed(4)
        send(10).start()
        send(11).start()
        landed(5)
        send(13).start()
        landed(11)
        early_scores(6, s3)

    @pl.when(step == LATE)
    def _():
        landed(6)
        send(14).start()
        q_landed(0)
        for n in (4, 6, 5):
            q_send_of(n).start()
        for kind in (7, 8, 13, 14):
            landed(kind)

    @pl.when(step == LATE + 1)
    def _():
        landed(2)
        send(12).start()

    @pl.when(step == DEC)
    def _():
        landed(10)
        landed(12)
        for i in range(15):
            send(i).wait_send()
        wk_copy().wait()
        wv_copy().wait()
        for n in range(1, 7):
            q_landed(n)
        for n in range(7):
            q_send_of(n).wait_send()
        sel = selbuf[pl.ds(pl.multiple_of(span * DOCS, DOCS), DOCS), :].astype(BF)
        chosen = nn_dot(sel, qall[...]).astype(BF)
        col = iota((DOCS, AUG), 1)
        doc = iota((DOCS, AUG), 0)
        last = FRESH + 2 * LAT
        for t in range(STEPS):
            at = pl.ds(16 * TOK + t * DOCS, DOCS)
            cb[at, 0:LAT] = chosen[:, FRESH + t * LAT : FRESH + (t + 1) * LAT]
            mark = jnp.where((col == doc) | ((col == 32) & (t == 1)), 1.0, 0.0)
            rope = chosen[:, last + t * ROPE : last + (t + 1) * ROPE].astype(F32)
            cb[at, LAT:WIDE] = jnp.concatenate([rope, mark], axis=1).astype(BF)
        pad = TOK - STEPS * DOCS
        cb[pl.ds(16 * TOK + STEPS * DOCS, pad), :] = jnp.where(
            iota((pad, WIDE), 1) == LAT + ROPE + 33, 1.0, 0.0
        ).astype(BF)
        row = iota((STEPS * DOCS, AUG), 0)
        dcol = iota((STEPS * DOCS, AUG), 1)
        wrong = ((dcol < 16) & (dcol != row % DOCS)) | ((dcol == 32) & (row < DOCS)) | (dcol == 33)
        daug = jnp.where(wrong, -BIG, 0.0)
        parts = []
        for j in range(4):
            nope = jnp.concatenate(
                [chosen[:, (j * 2 + t) * 128 : (j * 2 + t + 1) * 128] for t in range(STEPS)], axis=0
            )
            at = 1024 + j * 128
            rope = jnp.concatenate(
                [chosen[:, at + t * ROPE : at + (t + 1) * ROPE] for t in range(STEPS)], axis=0
            )
            lat = nn_dot(nope, wkd[j]).astype(BF)
            end = jnp.concatenate([rope.astype(F32), daug], axis=1).astype(BF)
            parts.append(jnp.concatenate([lat, end], axis=1))
        dq = jnp.concatenate(parts, axis=0)
        s = nt_dot(dq, cb[...])
        best = jnp.max(s, axis=1, keepdims=True)
        w = jnp.exp2((s - best) * EXPC)
        total = jnp.sum(w, axis=1, keepdims=True)
        acc = nn_dot(w.astype(BF), cb[:, pl.ds(0, LAT)])
        for j in range(4):
            rest = acc[j * 32 : (j + 1) * 32]
            split = []
            for _ in range(3):
                piece = rest.astype(BF)
                split.append(piece)
                rest = rest - piece.astype(F32)
            y = nn_dot(jnp.concatenate(split, axis=0), wvd[j])
            y = (y[0:32] + y[32:64] + y[64:96]) / total[j * 32 : (j + 1) * 32]
            y = y.astype(BF)
            for t in range(STEPS):
                do_own[t, :, j * VHEAD : (j + 1) * VHEAD] = y[t * DOCS : (t + 1) * DOCS]

    @pl.when(step == DEC + 2)
    def _():
        for off in range(1, NSPAN):
            o_copy(off).wait()
        selo = jnp.where(assign_ref[...] == span * DOCS + iota((DOCS, 128), 0), 1.0, 0.0).astype(BF)
        for t in range(STEPS):
            full = jnp.concatenate([doall[i, t] for i in range(NSPAN)], axis=0)
            so[t] = nn_dot(selo, full).astype(BF)

    @pl.when(step >= LATE)
    def _():
        base = (step - LATE) * GROUP * TOK
        count = GROUP // CH

        def at(n):
            return pl.ds(pl.multiple_of(base + n * CH * TOK, CH * TOK), CH * TOK)

        def score(n):
            return nt_dot(qa[at(n), :], cb[pl.ds(0, 4 * TOK), :])

        s_next = score(0)
        for n in range(count):
            s = s_next
            if n + 1 < count:
                s_next = score(n + 1)
            s = jnp.concatenate([s, s2[at(n), :], s3[at(n), :], s1[at(n), :]], axis=1)
            best = jnp.max(s, axis=1, keepdims=True)
            w = jnp.exp2((s - best) * EXPC)
            total = jnp.sum(w, axis=1, keepdims=True)
            o = (nn_dot(w.astype(BF), cb[pl.ds(0, 9 * TOK), pl.ds(0, LAT)]) / total).astype(BF)
            for j in range(CH):
                h = n * CH + j
                out_ref[:, h * VHEAD : (h + 1) * VHEAD] = nn_dot(
                    o[j * TOK : (j + 1) * TOK], wv_ref[h]
                ).astype(BF)

    @pl.when(step == DEC)
    def _():
        for off in (1, 7, 2, 6, 3, 5, 4):
            o_copy(off).start()
        doall[span] = do_own[...]

    @pl.when(step == DEC + 2)
    def _():
        for n in (3, 0, 6, 1, 5, 2, 4, 7):
            s_out(n).start()
        columns(me)[...] = so[...]

    @pl.when(step == LAST)
    def _():
        for n in range(7):
            s_landed(n)
            s_out(8 + n).start()
        for n in range(7, 15):
            s_landed(n)
        for n in range(15):
            s_out(n).wait_send()
        dec_ref[...] = outbuf[...]


def body(
    q_prefill, kv_latent, key_rope, segment_ids, assignment, absorb_key, absorb_value,
    q_decode, new_latent, new_rope,
):
    vmem = pl.BlockSpec(memory_space=pltpu.VMEM)
    hbm = pl.BlockSpec(memory_space=pl.ANY)
    out, dec = pl.pallas_call(
        kernel,
        grid=(LATE + NG,),
        out_shape=(
            jax.ShapeDtypeStruct((TOK, H * VHEAD), BF),
            jax.ShapeDtypeStruct((STEPS, DOCS, H * VHEAD), BF),
        ),
        in_specs=[vmem] * 7
        + [
            hbm,
            hbm,
            pl.BlockSpec((GROUP, NOPE + ROPE, TOK), lambda i: (jnp.minimum(i, NG - 1), 0, 0)),
            pl.BlockSpec((GROUP, NOPE, LAT), lambda i: (jnp.minimum(i, NG - 1), 0, 0)),
            pl.BlockSpec((GROUP, LAT, VHEAD), lambda i: (jnp.maximum(i - LATE, 0), 0, 0)),
        ],
        out_specs=(
            pl.BlockSpec((TOK, GROUP * VHEAD), lambda i: (0, jnp.maximum(i - LATE, 0))),
            pl.BlockSpec((STEPS, DOCS, H * VHEAD), lambda i: (0, 0, 0)),
        ),
        scratch_shapes=[
            pltpu.VMEM((17 * TOK, WIDE), BF),
            pltpu.VMEM((H * TOK, WIDE), BF),
            pltpu.VMEM((H * TOK, TOK), F32),
            pltpu.VMEM((H * TOK, 2 * TOK), F32),
            pltpu.VMEM((H * TOK, 2 * TOK), F32),
            pltpu.VMEM((AUG, TOK), BF),
            pltpu.VMEM((STEPS, DOCS * 8, NOPE), F32),
            pltpu.VMEM((STEPS, DOCS * 8, NOPE), F32),
            pltpu.VMEM((DOCS, QCOL), BF),
            pltpu.VMEM((NSPAN * DOCS, QCOL), BF),
            pltpu.VMEM((128, 128), F32),
            pltpu.VMEM((4, NOPE, LAT), BF),
            pltpu.VMEM((4, LAT, VHEAD), BF),
            pltpu.VMEM((STEPS, DOCS, 512), BF),
            pltpu.VMEM((NSPAN, STEPS, DOCS, 512), BF),
            pltpu.VMEM((STEPS, DOCS, 512), BF),
            pltpu.VMEM((STEPS, DOCS, H * VHEAD), BF),
            pltpu.SemaphoreType.DMA((15,)),
            pltpu.SemaphoreType.DMA((15,)),
            pltpu.SemaphoreType.DMA((7,)),
            pltpu.SemaphoreType.DMA((7,)),
            pltpu.SemaphoreType.DMA((7,)),
            pltpu.SemaphoreType.DMA((7,)),
            pltpu.SemaphoreType.DMA((15,)),
            pltpu.SemaphoreType.DMA((15,)),
            pltpu.SemaphoreType.DMA((2,)),
        ],
        compiler_params=pltpu.CompilerParams(
            dimension_semantics=("arbitrary",),
            collective_id=0,
            has_side_effects=True,
            vmem_limit_bytes=60 * 1024 * 1024,
        ),
    )(
        kv_latent[0], key_rope[0].T, segment_ids, assignment.reshape(1, 128), q_decode,
        new_latent, new_rope, absorb_key, absorb_value,
        q_prefill[0].transpose(1, 2, 0), absorb_key, absorb_value,
    )
    return (out[None], dec)


def solution(mesh):
    in_specs = (
        P("span", "seq", None, None),
        P("span", "seq", None),
        P("span", "seq", None),
        P(),
        P(),
        P(),
        P(),
        P(None, "span", None, None),
        P(None, "span", None),
        P(None, "span", None),
    )
    out_specs = (P("span", "seq", None), P(None, "span", None))
    return jax.shard_map(body, mesh=mesh, in_specs=in_specs, out_specs=out_specs, check_vma=False)
```

```python
import math

import jax
import jax.numpy as jnp
from jax import lax
from jax.experimental import pallas as pl
from jax.experimental.pallas import tpu as pltpu
from jax.sharding import PartitionSpec as P

H = 64
NOPE = 128
ROPE = 64
LAT = 512
VHEAD = 128
TOK = 128
DOCS = 16
STEPS = 2
NSEQ = 16
NSPAN = 8
WIDE = 640
AUG = 64
BIG = float(2.0**100)
EPS = 1e-06
SCALE = (NOPE + ROPE) ** (-0.5)
EXPC = SCALE * math.log2(math.e)
GROUP = 8
NG = H // GROUP
CH = 4
RELAY0 = 5
EARLY = NG
MIDDLE = NG + 1
LATE = NG + 2
DEC = LATE + 1
LAST = LATE + NG - 1
QCOL = 2688
FRESH = 1536
BF = jnp.bfloat16
F32 = jnp.float32
MESH = pl.DeviceIdType.MESH


def normed(values):
    values = values.astype(F32)
    mean = jnp.mean(values * values, axis=-1, keepdims=True)
    return values * lax.rsqrt(mean + EPS)


def iota(shape, dim):
    return lax.broadcasted_iota(jnp.int32, shape, dim)


def nt_dot(a, b):
    return lax.dot_general(a, b, (((1,), (1,)), ((), ())), preferred_element_type=F32)


def nn_dot(a, b):
    return jnp.dot(a, b, preferred_element_type=F32)


def kernel(
    lat_ref, rope_ref, seg_ref, assign_ref, qd_ref, nl_ref, nr_ref, wk_any, wv_any,
    q_ref, wk_ref, wv_ref,
    out_ref, dec_ref,
    cb, qa, s1, s2, s3, qaug, qf, qr, qm, qall, selbuf, wkd, wvd, do_own, doall, so, outbuf,
    g_send, g_recv, q_send, q_recv, o_send, o_recv, s_send, s_recv, w_sem,
):
    step = pl.program_id(0)
    me = lax.axis_index("seq")
    span = lax.axis_index("span")
    z = me // 4
    yh = (me // 2) % 2
    k = me % 2
    zp = (z + 1) % 4
    zm = (z + 3) % 4
    z2 = (z + 2) % 4

    def idx(zz, yy, kk):
        return zz * 4 + yy * 2 + kk

    part = idx(z, yh, 1 - k)
    ypeer = idx(z, 1 - yh, k)
    up = idx(zp, yh, k)
    down = idx(zm, yh, k)

    def less(a, b):
        return (b - a + 31) // 32

    def rows(block, owner):
        slot = (block - owner + 24) % 16
        phase = owner % 4
        back = (owner // 4 - block // 4 + 4) % 4
        near = less(0, back) * less(back, 2)
        other = (block % 4 // 2 + phase // 2) % 2
        high = less(7 - phase, slot) * less(slot, 8)
        place = near * (4 + 2 * other + block % 2) + (1 - near) * (slot - 4 * high)
        return cb.at[pl.ds(pl.multiple_of(place * TOK, TOK), TOK)]

    kinds = [
        idx(z, 1 - yh, k),
        idx(zm, yh, k),
        idx(zp, yh, k),
        idx(zm, 1 - yh, k),
        idx(zp, 1 - yh, k),
        idx(z2, yh, k),
        idx(z2, 1 - yh, k),
    ]
    arrive = kinds + [part] + [b + 1 - 2 * k for b in kinds]

    def copy(src, dst, target, kind, number):
        return pltpu.make_async_remote_copy(
            src_ref=src,
            dst_ref=dst,
            send_sem=g_send.at[number],
            recv_sem=g_recv.at[kind],
            device_id=(target, span),
            device_id_type=MESH,
        )

    plan = [
        (me, ypeer, 0),
        (me, up, 1),
        (me, part, 7),
        (me, down, 2),
        (kinds[0], up, 3),
        (kinds[0], down, 4),
        (kinds[0], part, 8),
        (kinds[1], up, 5),
        (kinds[1], part, 9),
        (kinds[3], part, 11),
        (kinds[4], down, 6),
        (kinds[4], part, 12),
        (kinds[2], part, 10),
        (kinds[5], part, 13),
        (kinds[6], part, 14),
    ]

    def send(i):
        block, target, kind = plan[i]
        return copy(rows(block, me), rows(block, target), target, kind, i)

    def landed(kind):
        dst = rows(arrive[kind], me)
        copy(dst, dst, part, kind, 0).wait_recv()

    x = span // 2
    lo = span % 2
    lopeer = x * 2 + 1 - lo

    def qrows(src):
        return qall.at[pl.ds(pl.multiple_of(src * DOCS, DOCS), DOCS)]

    def q_copy(src, dst, target, number):
        return pltpu.make_async_remote_copy(
            src_ref=src,
            dst_ref=dst,
            send_sem=q_send.at[number],
            recv_sem=q_recv.at[number],
            device_id=(me, target),
            device_id_type=MESH,
        )

    def q_send_of(number):
        if number == 0:
            return q_copy(qm, qrows(span), lopeer, 0)
        xx = (x + (number - 1) % 3 + 1) % 4
        if number <= 3:
            return q_copy(qm, qrows(span), xx * 2 + lo, number)
        return q_copy(qrows(lopeer), qrows(lopeer), xx * 2 + lo, number)

    def q_landed(number):
        if number == 0:
            src = lopeer
        else:
            xx = (x + 3 - (number - 1) % 3) % 4
            src = xx * 2 + (lo if number <= 3 else 1 - lo)
        q_copy(qrows(src), qrows(src), lopeer, number).wait_recv()

    def o_copy(off):
        return pltpu.make_async_remote_copy(
            src_ref=do_own,
            dst_ref=doall.at[span],
            send_sem=o_send.at[off - 1],
            recv_sem=o_recv.at[off - 1],
            device_id=(me, (span + off) % NSPAN),
            device_id_type=MESH,
        )

    def columns(block):
        return outbuf.at[:, :, pl.ds(pl.multiple_of(block * 512, 512), 512)]

    def s_copy(src, dst, target, number):
        return pltpu.make_async_remote_copy(
            src_ref=src,
            dst_ref=dst,
            send_sem=s_send.at[number],
            recv_sem=s_recv.at[number],
            device_id=(target, span),
            device_id_type=MESH,
        )

    def chip(off):
        return ((me // 2 + off) % 8) * 2 + k

    def s_out(number):
        if number == 7:
            return s_copy(so, columns(me), part, 7)
        if number < 7:
            return s_copy(so, columns(me), chip(number + 1), number)
        block = chip(8 - (number - 7))
        return s_copy(columns(block), columns(block), part, number)

    def s_landed(number):
        if number == 7:
            block = part
        elif number < 7:
            block = chip(8 - (number + 1))
        else:
            block = chip(8 - (number - 7)) + 1 - 2 * k
        s_copy(columns(block), columns(block), part, number).wait_recv()

    wk_copy = lambda: pltpu.make_async_copy(wk_any.at[pl.ds(me * 4, 4)], wkd, w_sem.at[0])
    wv_copy = lambda: pltpu.make_async_copy(wv_any.at[pl.ds(me * 4, 4)], wvd, w_sem.at[1])

    @pl.when(step == 0)
    def _():
        barrier = pltpu.get_barrier_semaphore()
        for off in range(1, NSEQ):
            pl.semaphore_signal(
                barrier, inc=1, device_id=((me + off) % NSEQ, span), device_id_type=MESH
            )
        for off in range(1, NSPAN):
            pl.semaphore_signal(
                barrier, inc=1, device_id=(me, (span + off) % NSPAN), device_id_type=MESH
            )
        wk_copy().start()
        wv_copy().start()
        cb[pl.ds(8 * TOK, TOK), 0:LAT] = normed(lat_ref[...]).astype(BF)
        segs = seg_ref[:, pl.ds(pl.multiple_of(me * TOK, TOK), TOK)].astype(F32)
        seg = jnp.sum(jnp.where(iota((NSPAN, TOK), 0) == span, segs, 0.0), axis=0, keepdims=True)
        seg = seg.astype(jnp.int32)
        number = iota((AUG, TOK), 0)
        same = number == seg
        kaug = jnp.where(same | (number - 16 == me), 1.0, 0.0)
        late = (number >= 16) & (number < 32) & (number - 16 > me)
        wrong = ((number < 16) & jnp.logical_not(same)) | late
        qaug[...] = jnp.where(wrong, -BIG, 0.0).astype(BF)
        tail = jnp.concatenate([rope_ref[...].astype(F32), kaug], axis=0)
        cb[pl.ds(8 * TOK, TOK), LAT:WIDE] = tail.T.astype(BF)
        at8 = pl.ds(pl.multiple_of((me // 2) * 8, 8), 8)
        for t in range(STEPS):
            block = qd_ref[t, :, at8, :].astype(F32).reshape(DOCS * 8, NOPE + ROPE)
            qf[t] = block[:, 0:NOPE]
            qr[t, :, 0:ROPE] = block[:, NOPE:]
        for j in range(4):
            ropes = []
            for t in range(STEPS):
                pick = pl.ds(k * 4 + j, DOCS, stride=8)
                n = j * 2 + t
                qm[:, n * 128 : (n + 1) * 128] = qf.at[t][pick, :].astype(BF)
                ropes.append(qr.at[t][pick, :][:, 0:ROPE])
            qm[:, 1024 + j * 128 : 1024 + (j + 1) * 128] = jnp.concatenate(ropes, axis=1).astype(BF)
        for t in range(STEPS):
            qm[:, FRESH + t * LAT : FRESH + (t + 1) * LAT] = normed(nl_ref[t]).astype(BF)
        both = jnp.concatenate([nr_ref[0].astype(F32), nr_ref[1].astype(F32)], axis=1)
        qm[:, FRESH + 2 * LAT : QCOL] = both.astype(BF)
        pl.semaphore_wait(barrier, NSEQ + NSPAN - 2)
        for i in (1, 0, 2):
            send(i).start()
        for n in (1, 3, 2):
            q_send_of(n).start()
        qrows(span)[...] = qm[...]
        selbuf[...] = jnp.where(assign_ref[...] == iota((128, 128), 0), 1.0, 0.0).T

    @pl.when(step < NG)
    def _():
        own_keys = cb[pl.ds(8 * TOK, TOK), :]
        tri = jnp.where(iota((TOK, TOK), 0) >= iota((TOK, TOK), 1), 0.0, -1e30)
        first = pl.multiple_of(step * GROUP * TOK, GROUP * TOK)
        for j in range(GROUP):
            at = pl.ds(pl.multiple_of(first + j * TOK, TOK), TOK)
            nope = q_ref[j, 0:NOPE, :].T
            qa[at, 0:LAT] = nn_dot(nope, wk_ref[j]).astype(BF)
            qa[at, LAT:WIDE] = jnp.concatenate([q_ref[j, NOPE:, :], qaug[...]], axis=0).T
        for j in range(0, GROUP, 4):
            at = pl.ds(pl.multiple_of(first + j * TOK, 4 * TOK), 4 * TOK)
            s1[at, :] = nt_dot(qa[at, :], own_keys) + jnp.concatenate([tri] * 4, axis=0)

    @pl.when(step == RELAY0)
    def _():
        landed(1)
        send(7).start()
        send(8).start()

    def early_scores(place, dst):
        keys = cb[pl.ds(place * TOK, 2 * TOK), :]

        def chunk(n, carry):
            at = pl.ds(pl.multiple_of(n * 4 * TOK, 4 * TOK), 4 * TOK)
            dst[at, :] = nt_dot(qa[at, :], keys)
            return carry

        lax.fori_loop(0, H // 4, chunk, 0, unroll=4)

    @pl.when(step == EARLY)
    def _():
        landed(0)
        for i in (4, 5, 6, 3):
            send(i).start()
        q_send_of(0).start()
        landed(9)
        early_scores(4, s2)

    @pl.when(step == MIDDLE)
    def _():
        landed(3)
        send(9).start()
        landed(4)
        send(10).start()
        send(11).start()
        landed(5)
        send(13).start()
        q_landed(0)
        for n in (4, 6, 5):
            q_send_of(n).start()
        landed(11)
        early_scores(6, s3)

    @pl.when(step == LATE)
    def _():
        landed(6)
        send(14).start()
        landed(2)
        send(12).start()
        for kind in (7, 8, 13, 14):
            landed(kind)

    @pl.when(step == DEC)
    def _():
        landed(10)
        landed(12)
        for i in range(15):
            send(i).wait_send()
        wk_copy().wait()
        wv_copy().wait()
        for n in range(1, 7):
            q_landed(n)
        for n in range(7):
            q_send_of(n).wait_send()
        sel = selbuf[pl.ds(pl.multiple_of(span * DOCS, DOCS), DOCS), :].astype(BF)
        chosen = nn_dot(sel, qall[...]).astype(BF)
        col = iota((DOCS, AUG), 1)
        doc = iota((DOCS, AUG), 0)
        last = FRESH + 2 * LAT
        for t in range(STEPS):
            at = pl.ds(16 * TOK + t * DOCS, DOCS)
            cb[at, 0:LAT] = chosen[:, FRESH + t * LAT : FRESH + (t + 1) * LAT]
            mark = jnp.where((col == doc) | ((col == 32) & (t == 1)), 1.0, 0.0)
            rope = chosen[:, last + t * ROPE : last + (t + 1) * ROPE].astype(F32)
            cb[at, LAT:WIDE] = jnp.concatenate([rope, mark], axis=1).astype(BF)
        pad = TOK - STEPS * DOCS
        cb[pl.ds(16 * TOK + STEPS * DOCS, pad), :] = jnp.where(
            iota((pad, WIDE), 1) == LAT + ROPE + 33, 1.0, 0.0
        ).astype(BF)
        row = iota((STEPS * DOCS, AUG), 0)
        dcol = iota((STEPS * DOCS, AUG), 1)
        wrong = ((dcol < 16) & (dcol != row % DOCS)) | ((dcol == 32) & (row < DOCS)) | (dcol == 33)
        daug = jnp.where(wrong, -BIG, 0.0)
        parts = []
        for j in range(4):
            nope = jnp.concatenate(
                [chosen[:, (j * 2 + t) * 128 : (j * 2 + t + 1) * 128] for t in range(STEPS)], axis=0
            )
            at = 1024 + j * 128
            rope = jnp.concatenate(
                [chosen[:, at + t * ROPE : at + (t + 1) * ROPE] for t in range(STEPS)], axis=0
            )
            lat = nn_dot(nope, wkd[j]).astype(BF)
            end = jnp.concatenate([rope.astype(F32), daug], axis=1).astype(BF)
            parts.append(jnp.concatenate([lat, end], axis=1))
        dq = jnp.concatenate(parts, axis=0)
        s = nt_dot(dq, cb[...])
        best = jnp.max(s, axis=1, keepdims=True)
        w = jnp.exp2((s - best) * EXPC)
        total = jnp.sum(w, axis=1, keepdims=True)
        acc = nn_dot(w.astype(BF), cb[:, pl.ds(0, LAT)])
        for j in range(4):
            rest = acc[j * 32 : (j + 1) * 32]
            split = []
            for _ in range(3):
                piece = rest.astype(BF)
                split.append(piece)
                rest = rest - piece.astype(F32)
            y = nn_dot(jnp.concatenate(split, axis=0), wvd[j])
            y = (y[0:32] + y[32:64] + y[64:96]) / total[j * 32 : (j + 1) * 32]
            y = y.astype(BF)
            for t in range(STEPS):
                do_own[t, :, j * VHEAD : (j + 1) * VHEAD] = y[t * DOCS : (t + 1) * DOCS]

    @pl.when(step == DEC + 2)
    def _():
        for off in range(1, NSPAN):
            o_copy(off).wait()
        selo = jnp.where(assign_ref[...] == span * DOCS + iota((DOCS, 128), 0), 1.0, 0.0).astype(BF)
        for t in range(STEPS):
            full = jnp.concatenate([doall[i, t] for i in range(NSPAN)], axis=0)
            so[t] = nn_dot(selo, full).astype(BF)

    @pl.when(step == LAST)
    def _():
        for n in range(7):
            s_landed(n)
            s_out(8 + n).start()

    @pl.when(step >= LATE)
    def _():
        base = (step - LATE) * GROUP * TOK
        count = GROUP // CH

        def at(n):
            return pl.ds(pl.multiple_of(base + n * CH * TOK, CH * TOK), CH * TOK)

        def score(n):
            return nt_dot(qa[at(n), :], cb[pl.ds(0, 4 * TOK), :])

        s_next = score(0)
        for n in range(count):
            s = s_next
            if n + 1 < count:
                s_next = score(n + 1)
            s = jnp.concatenate([s, s2[at(n), :], s3[at(n), :], s1[at(n), :]], axis=1)
            best = jnp.max(s, axis=1, keepdims=True)
            w = jnp.exp2((s - best) * EXPC)
            total = jnp.sum(w, axis=1, keepdims=True)
            o = (nn_dot(w.astype(BF), cb[pl.ds(0, 9 * TOK), pl.ds(0, LAT)]) / total).astype(BF)
            for j in range(CH):
                h = n * CH + j
                out_ref[:, h * VHEAD : (h + 1) * VHEAD] = nn_dot(
                    o[j * TOK : (j + 1) * TOK], wv_ref[h]
                ).astype(BF)

    @pl.when(step == DEC)
    def _():
        for off in (1, 7, 2, 6, 3, 5, 4):
            o_copy(off).start()
        doall[span] = do_own[...]

    @pl.when(step == DEC + 2)
    def _():
        for n in (3, 0, 6, 1, 5, 2, 4, 7):
            s_out(n).start()
        columns(me)[...] = so[...]

    @pl.when(step == LAST)
    def _():
        for n in range(7, 15):
            s_landed(n)
        for n in range(15):
            s_out(n).wait_send()
        dec_ref[...] = outbuf[...]


def body(
    q_prefill, kv_latent, key_rope, segment_ids, assignment, absorb_key, absorb_value,
    q_decode, new_latent, new_rope,
):
    vmem = pl.BlockSpec(memory_space=pltpu.VMEM)
    hbm = pl.BlockSpec(memory_space=pl.ANY)
    out, dec = pl.pallas_call(
        kernel,
        grid=(LATE + NG,),
        out_shape=(
            jax.ShapeDtypeStruct((TOK, H * VHEAD), BF),
            jax.ShapeDtypeStruct((STEPS, DOCS, H * VHEAD), BF),
        ),
        in_specs=[vmem] * 7
        + [
            hbm,
            hbm,
            pl.BlockSpec((GROUP, NOPE + ROPE, TOK), lambda i: (jnp.minimum(i, NG - 1), 0, 0)),
            pl.BlockSpec((GROUP, NOPE, LAT), lambda i: (jnp.minimum(i, NG - 1), 0, 0)),
            pl.BlockSpec((GROUP, LAT, VHEAD), lambda i: (jnp.maximum(i - LATE, 0), 0, 0)),
        ],
        out_specs=(
            pl.BlockSpec((TOK, GROUP * VHEAD), lambda i: (0, jnp.maximum(i - LATE, 0))),
            pl.BlockSpec((STEPS, DOCS, H * VHEAD), lambda i: (0, 0, 0)),
        ),
        scratch_shapes=[
            pltpu.VMEM((17 * TOK, WIDE), BF),
            pltpu.VMEM((H * TOK, WIDE), BF),
            pltpu.VMEM((H * TOK, TOK), F32),
            pltpu.VMEM((H * TOK, 2 * TOK), F32),
            pltpu.VMEM((H * TOK, 2 * TOK), F32),
            pltpu.VMEM((AUG, TOK), BF),
            pltpu.VMEM((STEPS, DOCS * 8, NOPE), F32),
            pltpu.VMEM((STEPS, DOCS * 8, NOPE), F32),
            pltpu.VMEM((DOCS, QCOL), BF),
            pltpu.VMEM((NSPAN * DOCS, QCOL), BF),
            pltpu.VMEM((128, 128), F32),
            pltpu.VMEM((4, NOPE, LAT), BF),
            pltpu.VMEM((4, LAT, VHEAD), BF),
            pltpu.VMEM((STEPS, DOCS, 512), BF),
            pltpu.VMEM((NSPAN, STEPS, DOCS, 512), BF),
            pltpu.VMEM((STEPS, DOCS, 512), BF),
            pltpu.VMEM((STEPS, DOCS, H * VHEAD), BF),
            pltpu.SemaphoreType.DMA((15,)),
            pltpu.SemaphoreType.DMA((15,)),
            pltpu.SemaphoreType.DMA((7,)),
            pltpu.SemaphoreType.DMA((7,)),
            pltpu.SemaphoreType.DMA((7,)),
            pltpu.SemaphoreType.DMA((7,)),
            pltpu.SemaphoreType.DMA((15,)),
            pltpu.SemaphoreType.DMA((15,)),
            pltpu.SemaphoreType.DMA((2,)),
        ],
        compiler_params=pltpu.CompilerParams(
            dimension_semantics=("arbitrary",),
            collective_id=0,
            has_side_effects=True,
            vmem_limit_bytes=60 * 1024 * 1024,
        ),
    )(
        kv_latent[0], key_rope[0].T, segment_ids, assignment.reshape(1, 128), q_decode,
        new_latent, new_rope, absorb_key, absorb_value,
        q_prefill[0].transpose(1, 2, 0), absorb_key, absorb_value,
    )
    return (out[None], dec)


def solution(mesh):
    in_specs = (
        P("span", "seq", None, None),
        P("span", "seq", None),
        P("span", "seq", None),
        P(),
        P(),
        P(),
        P(),
        P(None, "span", None, None),
        P(None, "span", None),
        P(None, "span", None),
    )
    out_specs = (P("span", "seq", None), P(None, "span", None))
    return jax.shard_map(body, mesh=mesh, in_specs=in_specs, out_specs=out_specs, check_vma=False)
```

```python
import math

import jax
import jax.numpy as jnp
from jax import lax
from jax.experimental import pallas as pl
from jax.experimental.pallas import tpu as pltpu
from jax.sharding import PartitionSpec as P

H = 64
NOPE = 128
ROPE = 64
LAT = 512
VHEAD = 128
TOK = 128
HALF = 64
DOCS = 16
STEPS = 2
NSEQ = 16
NSPAN = 8
WIDE = 640
AUG = 64
BIG = float(2.0**100)
EPS = 1e-06
SCALE = (NOPE + ROPE) ** (-0.5)
EXPC = SCALE * math.log2(math.e)
GROUP = 8
NG = H // GROUP
CH = 4
RELAY0 = 5
EARLY = NG
MIDDLE = NG + 1
LATE = NG + 2
DEC = LATE + 1
LAST = LATE + NG - 1
QCOL = 2688
FRESH = 1536
BF = jnp.bfloat16
F32 = jnp.float32
MESH = pl.DeviceIdType.MESH


def normed(values):
    values = values.astype(F32)
    mean = jnp.mean(values * values, axis=-1, keepdims=True)
    return values * lax.rsqrt(mean + EPS)


def iota(shape, dim):
    return lax.broadcasted_iota(jnp.int32, shape, dim)


def nt_dot(a, b):
    return lax.dot_general(a, b, (((1,), (1,)), ((), ())), preferred_element_type=F32)


def nn_dot(a, b):
    return jnp.dot(a, b, preferred_element_type=F32)


def kernel(
    lat_ref, rope_ref, seg_ref, assign_ref, qd_ref, nl_ref, nr_ref, wk_any, wv_any,
    q_ref, wk_ref, wv_ref,
    out_ref, dec_ref,
    cb, qa, s1, s2, s3, qaug, qf, qr, qm, qall, selbuf, wkd, wvd, do_own, doall, so, outbuf,
    g_send, g_recv, q_send, q_recv, o_send, o_recv, s_send, s_recv, w_sem,
):
    step = pl.program_id(0)
    me = lax.axis_index("seq")
    span = lax.axis_index("span")
    z = me // 4
    yh = (me // 2) % 2
    k = me % 2
    zp = (z + 1) % 4
    zm = (z + 3) % 4
    z2 = (z + 2) % 4

    def idx(zz, yy, kk):
        return zz * 4 + yy * 2 + kk

    part = idx(z, yh, 1 - k)
    ypeer = idx(z, 1 - yh, k)
    up = idx(zp, yh, k)
    down = idx(zm, yh, k)

    def less(a, b):
        return (b - a + 31) // 32

    def rows(block, owner, half):
        slot = (block - owner + 24) % 16
        phase = owner % 4
        back = (owner // 4 - block // 4 + 4) % 4
        near = less(0, back) * less(back, 2)
        other = (block % 4 // 2 + phase // 2) % 2
        high = less(7 - phase, slot) * less(slot, 8)
        place = near * (4 + 2 * other + block % 2) + (1 - near) * (slot - 4 * high)
        return cb.at[pl.ds(pl.multiple_of(place * TOK + half * HALF, HALF), HALF)]

    kinds = [
        idx(z, 1 - yh, k),
        idx(zm, yh, k),
        idx(zp, yh, k),
        idx(zm, 1 - yh, k),
        idx(zp, 1 - yh, k),
        idx(z2, yh, k),
        idx(z2, 1 - yh, k),
    ]
    arrive = kinds + [part] + [b + 1 - 2 * k for b in kinds]

    def copy(src, dst, target, kind, number, half):
        return pltpu.make_async_remote_copy(
            src_ref=src,
            dst_ref=dst,
            send_sem=g_send.at[2 * number + half],
            recv_sem=g_recv.at[2 * kind + half],
            device_id=(target, span),
            device_id_type=MESH,
        )

    plan = [
        (me, ypeer, 0),
        (me, up, 1),
        (me, part, 7),
        (me, down, 2),
        (kinds[0], up, 3),
        (kinds[0], down, 4),
        (kinds[0], part, 8),
        (kinds[1], up, 5),
        (kinds[1], part, 9),
        (kinds[3], part, 11),
        (kinds[4], down, 6),
        (kinds[4], part, 12),
        (kinds[2], part, 10),
        (kinds[5], part, 13),
        (kinds[6], part, 14),
    ]

    def send(i, half):
        block, target, kind = plan[i]
        return copy(rows(block, me, half), rows(block, target, half), target, kind, i, half)

    def go(*numbers, halves=(0, 1)):
        for half in halves:
            for i in numbers:
                send(i, half).start()

    def landed(kind, halves=(0, 1)):
        for half in halves:
            dst = rows(arrive[kind], me, half)
            copy(dst, dst, part, kind, 0, half).wait_recv()

    x = span // 2
    lo = span % 2
    lopeer = x * 2 + 1 - lo

    def qrows(src):
        return qall.at[pl.ds(pl.multiple_of(src * DOCS, DOCS), DOCS)]

    def q_copy(src, dst, target, number):
        return pltpu.make_async_remote_copy(
            src_ref=src,
            dst_ref=dst,
            send_sem=q_send.at[number],
            recv_sem=q_recv.at[number],
            device_id=(me, target),
            device_id_type=MESH,
        )

    def q_send_of(number):
        if number == 0:
            return q_copy(qm, qrows(span), lopeer, 0)
        xx = (x + (number - 1) % 3 + 1) % 4
        if number <= 3:
            return q_copy(qm, qrows(span), xx * 2 + lo, number)
        return q_copy(qrows(lopeer), qrows(lopeer), xx * 2 + lo, number)

    def q_landed(number):
        if number == 0:
            src = lopeer
        else:
            xx = (x + 3 - (number - 1) % 3) % 4
            src = xx * 2 + (lo if number <= 3 else 1 - lo)
        q_copy(qrows(src), qrows(src), lopeer, number).wait_recv()

    def o_copy(off):
        return pltpu.make_async_remote_copy(
            src_ref=do_own,
            dst_ref=doall.at[span],
            send_sem=o_send.at[off - 1],
            recv_sem=o_recv.at[off - 1],
            device_id=(me, (span + off) % NSPAN),
            device_id_type=MESH,
        )

    def columns(block):
        return outbuf.at[:, :, pl.ds(pl.multiple_of(block * 512, 512), 512)]

    def s_copy(src, dst, target, number):
        return pltpu.make_async_remote_copy(
            src_ref=src,
            dst_ref=dst,
            send_sem=s_send.at[number],
            recv_sem=s_recv.at[number],
            device_id=(target, span),
            device_id_type=MESH,
        )

    def chip(off):
        return ((me // 2 + off) % 8) * 2 + k

    def s_out(number):
        if number == 7:
            return s_copy(so, columns(me), part, 7)
        if number < 7:
            return s_copy(so, columns(me), chip(number + 1), number)
        block = chip(8 - (number - 7))
        return s_copy(columns(block), columns(block), part, number)

    def s_landed(number):
        if number == 7:
            block = part
        elif number < 7:
            block = chip(8 - (number + 1))
        else:
            block = chip(8 - (number - 7)) + 1 - 2 * k
        s_copy(columns(block), columns(block), part, number).wait_recv()

    wk_copy = lambda: pltpu.make_async_copy(wk_any.at[pl.ds(me * 4, 4)], wkd, w_sem.at[0])
    wv_copy = lambda: pltpu.make_async_copy(wv_any.at[pl.ds(me * 4, 4)], wvd, w_sem.at[1])

    @pl.when(step == 0)
    def _():
        barrier = pltpu.get_barrier_semaphore()
        for off in range(1, NSEQ):
            pl.semaphore_signal(
                barrier, inc=1, device_id=((me + off) % NSEQ, span), device_id_type=MESH
            )
        for off in range(1, NSPAN):
            pl.semaphore_signal(
                barrier, inc=1, device_id=(me, (span + off) % NSPAN), device_id_type=MESH
            )
        wk_copy().start()
        wv_copy().start()
        cb[pl.ds(8 * TOK, TOK), 0:LAT] = normed(lat_ref[...]).astype(BF)
        segs = seg_ref[:, pl.ds(pl.multiple_of(me * TOK, TOK), TOK)].astype(F32)
        seg = jnp.sum(jnp.where(iota((NSPAN, TOK), 0) == span, segs, 0.0), axis=0, keepdims=True)
        seg = seg.astype(jnp.int32)
        number = iota((AUG, TOK), 0)
        same = number == seg
        kaug = jnp.where(same | (number - 16 == me), 1.0, 0.0)
        late = (number >= 16) & (number < 32) & (number - 16 > me)
        wrong = ((number < 16) & jnp.logical_not(same)) | late
        qaug[...] = jnp.where(wrong, -BIG, 0.0).astype(BF)
        tail = jnp.concatenate([rope_ref[...].astype(F32), kaug], axis=0)
        cb[pl.ds(8 * TOK, TOK), LAT:WIDE] = tail.T.astype(BF)
        at8 = pl.ds(pl.multiple_of((me // 2) * 8, 8), 8)
        for t in range(STEPS):
            block = qd_ref[t, :, at8, :].astype(F32).reshape(DOCS * 8, NOPE + ROPE)
            qf[t] = block[:, 0:NOPE]
            qr[t, :, 0:ROPE] = block[:, NOPE:]
        for j in range(4):
            ropes = []
            for t in range(STEPS):
                pick = pl.ds(k * 4 + j, DOCS, stride=8)
                n = j * 2 + t
                qm[:, n * 128 : (n + 1) * 128] = qf.at[t][pick, :].astype(BF)
                ropes.append(qr.at[t][pick, :][:, 0:ROPE])
            qm[:, 1024 + j * 128 : 1024 + (j + 1) * 128] = jnp.concatenate(ropes, axis=1).astype(BF)
        for t in range(STEPS):
            qm[:, FRESH + t * LAT : FRESH + (t + 1) * LAT] = normed(nl_ref[t]).astype(BF)
        both = jnp.concatenate([nr_ref[0].astype(F32), nr_ref[1].astype(F32)], axis=1)
        qm[:, FRESH + 2 * LAT : QCOL] = both.astype(BF)
        pl.semaphore_wait(barrier, NSEQ + NSPAN - 2)
        go(1, 0, 2)
        for n in (1, 3, 2):
            q_send_of(n).start()
        qrows(span)[...] = qm[...]
        selbuf[...] = jnp.where(assign_ref[...] == iota((128, 128), 0), 1.0, 0.0).T

    @pl.when(step < NG)
    def _():
        own_keys = cb[pl.ds(8 * TOK, TOK), :]
        tri = jnp.where(iota((TOK, TOK), 0) >= iota((TOK, TOK), 1), 0.0, -1e30)
        first = pl.multiple_of(step * GROUP * TOK, GROUP * TOK)
        for j in range(GROUP):
            at = pl.ds(pl.multiple_of(first + j * TOK, TOK), TOK)
            nope = q_ref[j, 0:NOPE, :].T
            qa[at, 0:LAT] = nn_dot(nope, wk_ref[j]).astype(BF)
            qa[at, LAT:WIDE] = jnp.concatenate([q_ref[j, NOPE:, :], qaug[...]], axis=0).T
        for j in range(0, GROUP, 4):
            at = pl.ds(pl.multiple_of(first + j * TOK, 4 * TOK), 4 * TOK)
            s1[at, :] = nt_dot(qa[at, :], own_keys) + jnp.concatenate([tri] * 4, axis=0)

    @pl.when(step == RELAY0)
    def _():
        landed(1)
        go(7, 8)

    def early_scores(place, dst):
        keys = cb[pl.ds(place * TOK, 2 * TOK), :]

        def chunk(n, carry):
            at = pl.ds(pl.multiple_of(n * 4 * TOK, 4 * TOK), 4 * TOK)
            dst[at, :] = nt_dot(qa[at, :], keys)
            return carry

        lax.fori_loop(0, H // 4, chunk, 0, unroll=4)

    @pl.when(step == EARLY)
    def _():
        landed(0, (0,))
        go(4, 5, 6, halves=(0,))
        landed(9)
        early_scores(4, s2)
        landed(0, (1,))
        go(4, 5, 6, halves=(1,))
        go(3)
        q_send_of(0).start()

    @pl.when(step == MIDDLE)
    def _():
        for half in (0, 1):
            landed(4, (half,))
            go(10, 11, halves=(half,))
            landed(3, (half,))
            go(9, halves=(half,))
        landed(5)
        go(13)
        q_landed(0)
        for n in (4, 6, 5):
            q_send_of(n).start()
        landed(11)
        early_scores(6, s3)

    @pl.when(step == LATE)
    def _():
        for half in (0, 1):
            landed(6, (half,))
            go(14, halves=(half,))
        landed(2)
        go(12)
        for kind in (7, 8, 13, 14):
            landed(kind)

    @pl.when(step == DEC)
    def _():
        landed(10)
        landed(12)
        for i in range(15):
            for half in (0, 1):
                send(i, half).wait_send()
        wk_copy().wait()
        wv_copy().wait()
        for n in range(1, 7):
            q_landed(n)
        for n in range(7):
            q_send_of(n).wait_send()
        sel = selbuf[pl.ds(pl.multiple_of(span * DOCS, DOCS), DOCS), :].astype(BF)
        chosen = nn_dot(sel, qall[...]).astype(BF)
        col = iota((DOCS, AUG), 1)
        doc = iota((DOCS, AUG), 0)
        last = FRESH + 2 * LAT
        for t in range(STEPS):
            at = pl.ds(16 * TOK + t * DOCS, DOCS)
            cb[at, 0:LAT] = chosen[:, FRESH + t * LAT : FRESH + (t + 1) * LAT]
            mark = jnp.where((col == doc) | ((col == 32) & (t == 1)), 1.0, 0.0)
            rope = chosen[:, last + t * ROPE : last + (t + 1) * ROPE].astype(F32)
            cb[at, LAT:WIDE] = jnp.concatenate([rope, mark], axis=1).astype(BF)
        pad = TOK - STEPS * DOCS
        cb[pl.ds(16 * TOK + STEPS * DOCS, pad), :] = jnp.where(
            iota((pad, WIDE), 1) == LAT + ROPE + 33, 1.0, 0.0
        ).astype(BF)
        row = iota((STEPS * DOCS, AUG), 0)
        dcol = iota((STEPS * DOCS, AUG), 1)
        wrong = ((dcol < 16) & (dcol != row % DOCS)) | ((dcol == 32) & (row < DOCS)) | (dcol == 33)
        daug = jnp.where(wrong, -BIG, 0.0)
        parts = []
        for j in range(4):
            nope = jnp.concatenate(
                [chosen[:, (j * 2 + t) * 128 : (j * 2 + t + 1) * 128] for t in range(STEPS)], axis=0
            )
            at = 1024 + j * 128
            rope = jnp.concatenate(
                [chosen[:, at + t * ROPE : at + (t + 1) * ROPE] for t in range(STEPS)], axis=0
            )
            lat = nn_dot(nope, wkd[j]).astype(BF)
            end = jnp.concatenate([rope.astype(F32), daug], axis=1).astype(BF)
            parts.append(jnp.concatenate([lat, end], axis=1))
        dq = jnp.concatenate(parts, axis=0)
        s = nt_dot(dq, cb[...])
        best = jnp.max(s, axis=1, keepdims=True)
        w = jnp.exp2((s - best) * EXPC)
        total = jnp.sum(w, axis=1, keepdims=True)
        acc = nn_dot(w.astype(BF), cb[:, pl.ds(0, LAT)])
        for j in range(4):
            rest = acc[j * 32 : (j + 1) * 32]
            split = []
            for _ in range(3):
                piece = rest.astype(BF)
                split.append(piece)
                rest = rest - piece.astype(F32)
            y = nn_dot(jnp.concatenate(split, axis=0), wvd[j])
            y = (y[0:32] + y[32:64] + y[64:96]) / total[j * 32 : (j + 1) * 32]
            y = y.astype(BF)
            for t in range(STEPS):
                do_own[t, :, j * VHEAD : (j + 1) * VHEAD] = y[t * DOCS : (t + 1) * DOCS]

    @pl.when(step == DEC + 2)
    def _():
        for off in range(1, NSPAN):
            o_copy(off).wait()
        selo = jnp.where(assign_ref[...] == span * DOCS + iota((DOCS, 128), 0), 1.0, 0.0).astype(BF)
        for t in range(STEPS):
            full = jnp.concatenate([doall[i, t] for i in range(NSPAN)], axis=0)
            so[t] = nn_dot(selo, full).astype(BF)

    @pl.when(step == LAST)
    def _():
        for n in range(7):
            s_landed(n)
            s_out(8 + n).start()

    @pl.when(step >= LATE)
    def _():
        base = (step - LATE) * GROUP * TOK
        count = GROUP // CH

        def at(n):
            return pl.ds(pl.multiple_of(base + n * CH * TOK, CH * TOK), CH * TOK)

        def score(n):
            return nt_dot(qa[at(n), :], cb[pl.ds(0, 4 * TOK), :])

        s_next = score(0)
        for n in range(count):
            s = s_next
            if n + 1 < count:
                s_next = score(n + 1)
            s = jnp.concatenate([s, s2[at(n), :], s3[at(n), :], s1[at(n), :]], axis=1)
            best = jnp.max(s, axis=1, keepdims=True)
            w = jnp.exp2((s - best) * EXPC)
            total = jnp.sum(w, axis=1, keepdims=True)
            o = (nn_dot(w.astype(BF), cb[pl.ds(0, 9 * TOK), pl.ds(0, LAT)]) / total).astype(BF)
            for j in range(CH):
                h = n * CH + j
                out_ref[:, h * VHEAD : (h + 1) * VHEAD] = nn_dot(
                    o[j * TOK : (j + 1) * TOK], wv_ref[h]
                ).astype(BF)

    @pl.when(step == DEC)
    def _():
        for off in (1, 7, 2, 6, 3, 5, 4):
            o_copy(off).start()
        doall[span] = do_own[...]

    @pl.when(step == DEC + 2)
    def _():
        for n in (3, 0, 6, 1, 5, 2, 4, 7):
            s_out(n).start()
        columns(me)[...] = so[...]

    @pl.when(step == LAST)
    def _():
        for n in range(7, 15):
            s_landed(n)
        for n in range(15):
            s_out(n).wait_send()
        dec_ref[...] = outbuf[...]


def body(
    q_prefill, kv_latent, key_rope, segment_ids, assignment, absorb_key, absorb_value,
    q_decode, new_latent, new_rope,
):
    vmem = pl.BlockSpec(memory_space=pltpu.VMEM)
    hbm = pl.BlockSpec(memory_space=pl.ANY)
    out, dec = pl.pallas_call(
        kernel,
        grid=(LATE + NG,),
        out_shape=(
            jax.ShapeDtypeStruct((TOK, H * VHEAD), BF),
            jax.ShapeDtypeStruct((STEPS, DOCS, H * VHEAD), BF),
        ),
        in_specs=[vmem] * 7
        + [
            hbm,
            hbm,
            pl.BlockSpec((GROUP, NOPE + ROPE, TOK), lambda i: (jnp.minimum(i, NG - 1), 0, 0)),
            pl.BlockSpec((GROUP, NOPE, LAT), lambda i: (jnp.minimum(i, NG - 1), 0, 0)),
            pl.BlockSpec((GROUP, LAT, VHEAD), lambda i: (jnp.maximum(i - LATE, 0), 0, 0)),
        ],
        out_specs=(
            pl.BlockSpec((TOK, GROUP * VHEAD), lambda i: (0, jnp.maximum(i - LATE, 0))),
            pl.BlockSpec((STEPS, DOCS, H * VHEAD), lambda i: (0, 0, 0)),
        ),
        scratch_shapes=[
            pltpu.VMEM((17 * TOK, WIDE), BF),
            pltpu.VMEM((H * TOK, WIDE), BF),
            pltpu.VMEM((H * TOK, TOK), F32),
            pltpu.VMEM((H * TOK, 2 * TOK), F32),
            pltpu.VMEM((H * TOK, 2 * TOK), F32),
            pltpu.VMEM((AUG, TOK), BF),
            pltpu.VMEM((STEPS, DOCS * 8, NOPE), F32),
            pltpu.VMEM((STEPS, DOCS * 8, NOPE), F32),
            pltpu.VMEM((DOCS, QCOL), BF),
            pltpu.VMEM((NSPAN * DOCS, QCOL), BF),
            pltpu.VMEM((128, 128), F32),
            pltpu.VMEM((4, NOPE, LAT), BF),
            pltpu.VMEM((4, LAT, VHEAD), BF),
            pltpu.VMEM((STEPS, DOCS, 512), BF),
            pltpu.VMEM((NSPAN, STEPS, DOCS, 512), BF),
            pltpu.VMEM((STEPS, DOCS, 512), BF),
            pltpu.VMEM((STEPS, DOCS, H * VHEAD), BF),
            pltpu.SemaphoreType.DMA((30,)),
            pltpu.SemaphoreType.DMA((30,)),
            pltpu.SemaphoreType.DMA((7,)),
            pltpu.SemaphoreType.DMA((7,)),
            pltpu.SemaphoreType.DMA((7,)),
            pltpu.SemaphoreType.DMA((7,)),
            pltpu.SemaphoreType.DMA((15,)),
            pltpu.SemaphoreType.DMA((15,)),
            pltpu.SemaphoreType.DMA((2,)),
        ],
        compiler_params=pltpu.CompilerParams(
            dimension_semantics=("arbitrary",),
            collective_id=0,
            has_side_effects=True,
            vmem_limit_bytes=60 * 1024 * 1024,
        ),
    )(
        kv_latent[0], key_rope[0].T, segment_ids, assignment.reshape(1, 128), q_decode,
        new_latent, new_rope, absorb_key, absorb_value,
        q_prefill[0].transpose(1, 2, 0), absorb_key, absorb_value,
    )
    return (out[None], dec)


def solution(mesh):
    in_specs = (
        P("span", "seq", None, None),
        P("span", "seq", None),
        P("span", "seq", None),
        P(),
        P(),
        P(),
        P(),
        P(None, "span", None, None),
        P(None, "span", None),
        P(None, "span", None),
    )
    out_specs = (P("span", "seq", None), P(None, "span", None))
    return jax.shard_map(body, mesh=mesh, in_specs=in_specs, out_specs=out_specs, check_vma=False)
```
